256 devices in a mesh: kpt: 16 (over y, x), pw: 16 (over z, core).
Axes of the slice: x: 4, y: 4, z: 8, core: 2. Of those that a mesh axis runs over, the one named last changes fastest.
Arguments:
- energies: float32 [64, 512], P('kpt', 'pw'), may hold values from 0.5 to 3
- current: float32 [2, 64, 512], P(None, 'kpt', 'pw'), may hold values from -40 to 40
- previous: float32 [2, 64, 512], P(None, 'kpt', 'pw'), may hold values from -6 to 6
- previous_beta: float32 [2], replicated, may hold values from 0.5 to 2
- pair_left: bfloat16 [64, 512, 4096], P('kpt', None, 'pw'), may hold values from -0.09375 to 0.09375
- pair_right: bfloat16 [64, 512, 4096], P('kpt', None, 'pw'), may hold values from -0.25 to 0.25
- screened: bfloat16 [64, 4096, 4096], P('kpt', 'pw'), may hold values from -0.01171875 to 0.01171875
- momentum_index: int32 [64, 64], replicated, may hold values from 0 to 63, each once within a row
Outputs:
- last_vector: float32 [2, 64, 512], P(None, 'kpt', 'pw')
- prior_vector: float32 [2, 64, 512], P(None, 'kpt', 'pw')
- alpha_terms: float32 [2, 3], replicated
- beta_terms: float32 [2, 3], replicated
The draws below stay inside these ranges and needn't reach their ends.
Inputs may be any that keep to these rules, and one draw needn't show every extreme that they name: Each row of momentum_index names every index from 0 to 63 once.
All inputs are finite; a program needn't handle non-finite values.
Results may differ from the reference program's by a relative error of at most 0.003.
Values may be sent and summed in bfloat16 or wider, within the bound.
A program may use at most 128 MiB of HBM per device.

```python
import math
import jax
import jax.numpy as jnp
from jax import lax

NK = 64
NC = 512
NG = 4096
NVEC = 2
STEPS = 3


def draw_current(key, part):
    normal_part = jnp.clip(jax.random.normal(key, (NVEC, NK, NC), jnp.float32), -4.0, 4.0)
    kpoint_frac = jnp.arange(NK, dtype=jnp.float32) / NK
    band_frac = jnp.arange(NC, dtype=jnp.float32) / NC
    values = normal_part
    kpoint_scale = 10.0 ** (kpoint_frac - 0.5)
    band_scale = 10.0 ** (band_frac - 0.5)
    return values * kpoint_scale[None, :, None] * band_scale[None, None, :]


def block_scale(stream_key, shape, pieces, smallest, high):
    def one(axis_at, blocks):
        steps = jax.random.uniform(jax.random.fold_in(jax.random.fold_in(stream_key, 6), axis_at), (blocks,), jnp.float32, smallest / len(pieces), high / len(pieces))
        return jnp.repeat(jnp.exp(steps), shape[axis_at] // blocks).reshape((-1,) + (1,) * (len(shape) - axis_at - 1))

    factor_of = one(*pieces[0])
    for cut in pieces[1:]:
        factor_of = factor_of * one(*cut)
    return factor_of


def centred(stream_key, dims, scale, reach, cuts=(), held_as=jnp.bfloat16):
    values = jax.random.normal(stream_key, dims, jnp.float32) * scale
    if len(cuts) > 0:
        values = block_scale(stream_key, dims, cuts, -0.22, 0.18) * values
    return jnp.clip(values, min=-reach, max=reach).astype(held_as)


def setup_inputs(seed: int = 0) -> dict:
    key_list = jax.random.split(jax.random.key(seed), 9)
    energies = jnp.clip(0.5 + 2.5 * jax.random.uniform(key_list[0], (NK, NC), jnp.float32) ** block_scale(key_list[0], (NK, NC), ((0, 16), (1, 16)), -0.2, 0.2), 0.5, 3.0)
    current = draw_current(jax.random.fold_in(key_list[8], 71), 0)
    previous = centred(key_list[2], (NVEC, NK, NC), 1.0, 6.0, ((1, 16), (2, 16)), jnp.float32)
    previous_beta = jnp.clip(jnp.exp(jax.random.uniform(key_list[3], (NVEC,), jnp.float32, math.log(0.5), math.log(2.0))), 0.5, 2.0)
    pair_left = centred(key_list[4], (NK, NC, NG), NG ** -0.5, 0.09375, ((0, 16), (2, 16)))
    pair_right = centred(key_list[5], (NK, NC, NG), NC ** -0.5, 0.25, ((0, 16), (2, 16)))
    screened = centred(key_list[6], (NK, NG, NG), (NK * NG) ** -0.5, 0.01171875, ((0, 16), (1, 16)))
    momentum_index = jax.vmap(lambda own: jax.random.permutation(own, NK))(jax.random.split(key_list[7], NK)).reshape((NK, NK)).astype(jnp.int32)
    return dict(energies=energies, current=current, previous=previous, previous_beta=previous_beta, pair_left=pair_left, pair_right=pair_right, screened=screened, momentum_index=momentum_index)


epsilon = 1e-06

def reference(energies, current, previous, previous_beta, pair_left, pair_right, screened, momentum_index):
    entries = NK * NC
    left_float = pair_left.astype(jnp.float32)
    right_float = pair_right.astype(jnp.float32)
    vector = current
    earlier = previous
    beta_before = previous_beta
    alpha_list = []
    beta_list = []
    for turn_index in range(STEPS):
        rounded = vector.astype(jnp.bfloat16)
        density = jnp.einsum('kcg,vkc->kvg', right_float, rounded.astype(jnp.float32), precision=lax.Precision.HIGHEST).astype(jnp.bfloat16)
        columns = density.reshape(NK * NVEC, NG).T

        def add_transfer(running, qpoint):
            images = jnp.dot(screened[qpoint], columns, preferred_element_type=jnp.float32).reshape(NG, NK, NVEC)
            selector = (momentum_index == qpoint).astype(jnp.float32)
            return (running + jnp.einsum('jk,gkv->jvg', selector, images, precision=lax.Precision.HIGHEST), None)
        potential, unused = lax.scan(add_transfer, jnp.zeros((NK, NVEC, NG), jnp.float32), jnp.arange(NK, dtype=jnp.int32))
        potential_bf = potential.astype(jnp.bfloat16)
        direct = jnp.einsum('kcg,kvg->vkc', left_float, potential_bf.astype(jnp.float32), precision=lax.Precision.HIGHEST)
        applied = energies[None] * vector - direct - beta_before[:, None, None] * earlier
        alpha_now = lax.optimization_barrier(jnp.sum(vector * applied, axis=(1, 2))) / entries
        residual = applied - alpha_now[:, None, None] * vector
        beta_now = jnp.sqrt(lax.optimization_barrier(jnp.sum(residual * residual, axis=(1, 2))) / entries + epsilon)
        earlier = vector
        vector = residual / beta_now[:, None, None]
        beta_before = beta_now
        alpha_list.append(alpha_now)
        beta_list.append(beta_now)
    return (vector, earlier, jnp.stack(alpha_list, axis=1), jnp.stack(beta_list, axis=1))
```

```python
import functools

import jax
import jax.numpy as jnp
from jax import lax
from jax.experimental import pallas as pl
from jax.experimental.pallas import tpu as pltpu
from jax.sharding import Mesh
from jax.sharding import PartitionSpec as P

STEPS = 3
KPT = ("kpt_0", "kpt_1")
PW = ("pw_0", "pw_1")
MESH = pl.DeviceIdType.MESH
F32 = jnp.float32
BF16 = jnp.bfloat16
NT = (((1,), (1,)), ((), ()))

epsilon = 1e-06


def kernel(
    sizes, pack, momentum, left, right, screened,
    last, prior, alphas, betas,
    left_v, right_v, screened_v, selector,
    pk, dens, gath, rows, images, field, field_in, half_out, half_in, direct_z, direct_c, sums,
    vec, old, levels, beta, state,
    load_sem, pk_send, pk_recv, dens_send, dens_recv, gath_send, gath_recv, fwd_send, fwd_recv,
    field_send, field_recv, pair_send, pair_recv, dz_send, dz_recv, dc_send, dc_recv,
    sums_send, sums_recv,
):
    ny, nx, nz = sizes
    na = ny * nx
    nq, width = screened.shape[0], screened.shape[1]
    bands = left.shape[1]
    half = bands // 2
    entries = momentum.shape[0] * bands
    y, x = lax.axis_index("kpt_0"), lax.axis_index("kpt_1")
    z, c = lax.axis_index("pw_0"), lax.axis_index("pw_1")
    other = 1 - c
    a = y * nx + x
    b = z * 2 + c

    def plane_peer(i):
        ty = lax.rem(y + i // nx, ny)
        tx = lax.rem(x + lax.rem(i, nx), nx)
        return ty * nx + tx, (ty, tx, z, c)

    def plane_source(i):
        ty = lax.rem(y + ny - i // nx, ny)
        tx = lax.rem(x + nx - lax.rem(i, nx), nx)
        return ty * nx + tx

    def z_peer(i):
        tz = lax.rem(z + i, nz)
        return tz, (y, x, tz, c)

    def pw_peer(i):
        t = lax.rem(b + i, nz * 2)
        return t, (y, x, t // 2, lax.rem(t, 2))

    partner = (y, x, z, other)

    loads = [
        pltpu.make_async_copy(right, right_v, load_sem.at[0]),
        pltpu.make_async_copy(left, left_v, load_sem.at[1]),
    ]
    for h in range(2):
        for t in range(nz):
            at = (t * 2 + h) * width
            loads.append(
                pltpu.make_async_copy(
                    screened.at[:, :, pl.ds(at, width)],
                    screened_v.at[h, :, :, pl.ds(t * width, width)],
                    load_sem.at[2 + h * nz + t],
                )
            )
    for copy in loads:
        copy.start()

    barrier = pltpu.get_barrier_semaphore()

    @pl.loop(1, na)
    def _(i):
        pl.semaphore_signal(barrier, inc=1, device_id=plane_peer(i)[1], device_id_type=MESH)

    @pl.loop(1, nz * 2)
    def _(i):
        pl.semaphore_signal(barrier, inc=1, device_id=pw_peer(i)[1], device_id_type=MESH)

    nr = na * 8
    nk = momentum.shape[0]
    row = lax.broadcasted_iota(jnp.int32, (nr, nk), 0)
    col = lax.broadcasted_iota(jnp.int32, (nr, nk), 1)
    spread = ((row // 8) * 4 + row % 4 == col).astype(F32).astype(BF16)
    index = momentum[...].astype(F32).astype(BF16)
    by_row = jnp.dot(spread, index, preferred_element_type=F32).astype(BF16)
    by_both = lax.dot_general(by_row, spread, NT, preferred_element_type=F32).astype(jnp.int32)
    r1 = lax.broadcasted_iota(jnp.int32, (nr, nr), 0)
    r2 = lax.broadcasted_iota(jnp.int32, (nr, nr), 1)
    same = (r1 // 4) % 2 == (r2 // 4) % 2
    for q in range(nq):
        hit = jnp.logical_and(by_both == a * nq + q, same)
        selector[:, q * nr : (q + 1) * nr] = jnp.where(hit, 1.0, 0.0).astype(BF16)

    pk[b] = pack[...]
    pl.semaphore_wait(barrier, na - 1 + nz * 2 - 1)

    def pk_copy(i):
        t, device = pw_peer(i)
        return pltpu.make_async_remote_copy(
            pk.at[b], pk.at[b], pk_send.at[t], pk_recv.at[b], device, device_id_type=MESH
        )

    def arrived(ref, sem):
        pltpu.make_async_copy(ref, ref, sem).wait()

    @pl.loop(1, nz * 2)
    def _(i):
        pk_copy(i).start()

    @pl.loop(1, nz * 2)
    def _(i):
        t, _d = pw_peer(i)
        arrived(pk.at[t], pk_recv.at[t])

    lane = lax.broadcasted_iota(jnp.int32, (8, 128), 1)
    for j in range(bands // 128):
        for field_at, ref in ((0, vec), (1, old), (2, levels)):
            total = jnp.zeros((8, 128), F32)
            for m in range(4):
                turned = pk[4 * j + m]
                shift = (32 * (m - field_at)) % 128
                if shift:
                    turned = pltpu.roll(turned, shift, 1)
                total = total + jnp.where(lane // 32 == m, turned, 0.0)
            ref[:, j * 128 : (j + 1) * 128] = total
    beta[...] = jnp.broadcast_to(pack[:, 96:97], (8, 128))

    def own_k(n, k):
        return lax.broadcasted_iota(jnp.int32, (8, n), 0) % 4 == k

    def density_of(t, values):
        high = values.astype(BF16).astype(F32)
        both = jnp.concatenate([high, values - high], axis=0).astype(BF16)
        total = jnp.zeros((8, width), F32)
        for k in range(4):
            out = jnp.dot(both, right_v[k], preferred_element_type=F32)
            total = total + jnp.where(own_k(width, k), out[0:8] + out[8:16], 0.0)
        dens[t, z] = total

        @pl.loop(1, nz)
        def _(i):
            tz, device = z_peer(i)
            pltpu.make_async_remote_copy(
                dens.at[t, z], dens.at[t, z], dens_send.at[t, tz], dens_recv.at[t, z],
                device, device_id_type=MESH,
            ).start()

    def density_arrived(t):
        @pl.loop(1, nz)
        def _(i):
            tz, _d = z_peer(i)
            arrived(dens.at[t, tz], dens_recv.at[t, tz])

    def per_row(tile, at):
        lane_row = tile[:, at : at + 1]
        first = lax.broadcasted_iota(jnp.int32, (8, 1), 0) < 4
        top = jnp.sum(jnp.where(first, lane_row, 0.0), axis=0, keepdims=True)
        low = jnp.sum(jnp.where(first, 0.0, lane_row), axis=0, keepdims=True)
        return jnp.where(first, top, low)

    loads[0].wait()
    density_of(0, vec[...])
    density_arrived(0)
    for tz in range(nz):
        state[:, tz * width : (tz + 1) * width] = dens[0, tz]

    def step(t, carry):
        alpha_row, beta_row = carry
        gath[t, c, a] = state[...].astype(BF16)

        @pl.loop(1, na)
        def _(i):
            ta, device = plane_peer(i)
            pltpu.make_async_remote_copy(
                gath.at[t, c, a], gath.at[t, c, a], gath_send.at[t, ta], gath_recv.at[t, a],
                device, device_id_type=MESH,
            ).start()

        def forward(ta):
            return pltpu.make_async_remote_copy(
                gath.at[t, c, ta], gath.at[t, c, ta], fwd_send.at[t, ta], fwd_recv.at[t, ta],
                partner, device_id_type=MESH,
            )

        forward(a).start()

        @pl.loop(1, na)
        def _(i):
            ta = plane_source(i)
            arrived(gath.at[t, c, ta], gath_recv.at[t, ta])
            forward(ta).start()

        @pl.when(t == 0)
        def _():
            for copy in loads[2:]:
                copy.wait()

        def half_images(h, first):
            wide = gath[t, h].astype(F32)
            rows[...] = wide.reshape(nr, nz * width).astype(BF16)
            for q in range(nq):
                out = lax.dot_general(
                    rows[...], screened_v[h, q], NT, preferred_element_type=F32
                )
                images[q] = out if first else images[q] + out

        half_images(c, True)

        @pl.loop(0, na)
        def _(ta):
            arrived(gath.at[t, other, ta], fwd_recv.at[t, ta])

        half_images(other, False)

        values = images[...].reshape(nq * nr, width)
        high = values.astype(BF16)
        low = (values - high.astype(F32)).astype(BF16)
        chosen = jnp.dot(selector[...], high, preferred_element_type=F32)
        chosen = chosen + jnp.dot(selector[...], low, preferred_element_type=F32)
        field[t] = chosen.reshape(na, 8, width)

        @pl.loop(1, na)
        def _(i):
            ta, device = plane_peer(i)
            pltpu.make_async_remote_copy(
                field.at[t, ta], field_in.at[t, a], field_send.at[t, ta], field_recv.at[t, a],
                device, device_id_type=MESH,
            ).start()

        field_in[t, a] = field[t, a]

        @pl.loop(1, na)
        def _(i):
            ta = plane_source(i)
            arrived(field_in.at[t, ta], field_recv.at[t, ta])

        potential = jnp.sum(field_in[t], axis=0).astype(BF16)

        @pl.when(t == 0)
        def _():
            loads[1].wait()

        partial = jnp.zeros((8, bands), F32)
        for k in range(4):
            out = lax.dot_general(potential, left_v[k], NT, preferred_element_type=F32)
            partial = partial + jnp.where(own_k(bands, k), out, 0.0)
        half_out[t, 0] = partial[:, :half]
        half_out[t, 1] = partial[:, half:]
        pair = pltpu.make_async_remote_copy(
            half_out.at[t, other], half_in.at[t], pair_send.at[t], pair_recv.at[t],
            partner, device_id_type=MESH,
        )
        pair.start()
        arrived(half_in.at[t], pair_recv.at[t])
        direct_z[t, z] = half_out[t, c] + half_in[t]

        @pl.loop(1, nz)
        def _(i):
            tz, device = z_peer(i)
            pltpu.make_async_remote_copy(
                direct_z.at[t, z], direct_z.at[t, z], dz_send.at[t, tz], dz_recv.at[t, z],
                device, device_id_type=MESH,
            ).start()

        @pl.loop(1, nz)
        def _(i):
            tz, _d = z_peer(i)
            arrived(direct_z.at[t, tz], dz_recv.at[t, tz])

        direct_c[t, c] = jnp.sum(direct_z[t], axis=0)
        whole = pltpu.make_async_remote_copy(
            direct_c.at[t, c], direct_c.at[t, c], dc_send.at[t], dc_recv.at[t],
            partner, device_id_type=MESH,
        )
        whole.start()
        arrived(direct_c.at[t, other], dc_recv.at[t])
        direct = jnp.concatenate([direct_c[t, 0], direct_c[t, 1]], axis=1)

        vector = vec[...]
        applied = levels[...] * vector - direct - beta[:, 0:1] * old[...]
        cross = jnp.sum(vector * applied, axis=1, keepdims=True)
        square = jnp.sum(applied * applied, axis=1, keepdims=True)
        norm = jnp.sum(vector * vector, axis=1, keepdims=True)
        sums[t, a] = jnp.where(lane == 0, cross, jnp.where(lane == 1, square, norm))

        @pl.loop(1, na)
        def _(i):
            ta, device = plane_peer(i)
            pltpu.make_async_remote_copy(
                sums.at[t, a], sums.at[t, a], sums_send.at[t, ta], sums_recv.at[t, a],
                device, device_id_type=MESH,
            ).start()

        @pl.when(t < STEPS - 1)
        def _():
            density_of(t + 1, applied)

        @pl.loop(1, na)
        def _(i):
            ta = plane_source(i)
            arrived(sums.at[t, ta], sums_recv.at[t, ta])

        total = jnp.sum(sums[t], axis=0)
        cross_mean = per_row(total, 0) / entries
        square_mean = per_row(total, 1) / entries
        norm_mean = per_row(total, 2) / entries
        alpha = cross_mean
        mean_square = square_mean - 2.0 * alpha * cross_mean + alpha * alpha * norm_mean
        scale = jnp.sqrt(jnp.maximum(mean_square, 0.0) + epsilon)
        old[...] = vector
        vec[...] = (applied - alpha * vector) / scale
        beta[...] = jnp.broadcast_to(scale, (8, 128))

        @pl.when(t < STEPS - 1)
        def _():
            density_arrived(t + 1)
            for tz in range(nz):
                at = slice(tz * width, (tz + 1) * width)
                state[:, at] = (dens[t + 1, tz] - alpha * state[:, at]) / scale

        return jnp.where(lane == t, alpha, alpha_row), jnp.where(lane == t, scale, beta_row)

    zero = jnp.zeros((8, 128), F32)
    alpha_row, beta_row = lax.fori_loop(0, STEPS, step, (zero, zero))
    for tile, ref in ((alpha_row, alphas), (beta_row, betas)):
        ref[0:1, :] = tile[0:1, :STEPS]
        ref[1:2, :] = tile[4:5, :STEPS]
    group = pl.ds(pl.multiple_of((b // 4) * 128, 128), 128)
    for source, ref in ((vec, last), (old, prior)):
        turned = pltpu.roll(source[:, group], lax.rem(128 - lax.rem(b, 4) * 32, 128), 1)
        ref[...] = turned[:, :32]

    def sent(ref, sem):
        pltpu.make_async_copy(ref, ref, sem).wait()

    @pl.loop(1, nz * 2)
    def _(i):
        sent(pk.at[b], pk_send.at[pw_peer(i)[0]])

    @pl.loop(0, STEPS)
    def _(t):
        @pl.loop(1, na)
        def _(i):
            ta = plane_peer(i)[0]
            sent(gath.at[t, c, a], gath_send.at[t, ta])
            sent(field.at[t, ta], field_send.at[t, ta])
            sent(sums.at[t, a], sums_send.at[t, ta])

        @pl.loop(0, na)
        def _(ta):
            sent(gath.at[t, c, ta], fwd_send.at[t, ta])

        @pl.loop(1, nz)
        def _(i):
            tz = z_peer(i)[0]
            sent(dens.at[t, z], dens_send.at[t, tz])
            sent(direct_z.at[t, z], dz_send.at[t, tz])

        sent(half_out.at[t, other], pair_send.at[t])
        sent(direct_c.at[t, c], dc_send.at[t])


def on_device(
    energies, current, previous, previous_beta, pair_left, pair_right, screened, momentum_index
):
    ny, nx, nz = lax.axis_size("kpt_0"), lax.axis_size("kpt_1"), lax.axis_size("pw_0")
    na = ny * nx
    nvec, own_k, own_c = current.shape
    rows = nvec * own_k
    bands, width = pair_left.shape[1:]
    nq = screened.shape[0]
    pack = jnp.concatenate(
        [
            current.reshape(rows, own_c),
            previous.reshape(rows, own_c),
            jnp.concatenate([energies, energies], axis=0),
            jnp.broadcast_to(previous_beta[:, None, None], current.shape).reshape(rows, own_c),
        ],
        axis=1,
    )
    dma = pltpu.SemaphoreType.DMA
    vmem = pl.BlockSpec(memory_space=pltpu.VMEM)
    hbm = pl.BlockSpec(memory_space=pl.ANY)
    last, prior, alphas, betas = pl.pallas_call(
        functools.partial(kernel, (ny, nx, nz)),
        out_shape=(
            jax.ShapeDtypeStruct((rows, own_c), F32),
            jax.ShapeDtypeStruct((rows, own_c), F32),
            jax.ShapeDtypeStruct((nvec, STEPS), F32),
            jax.ShapeDtypeStruct((nvec, STEPS), F32),
        ),
        in_specs=[vmem, vmem, hbm, hbm, hbm],
        out_specs=(vmem, vmem, vmem, vmem),
        scratch_shapes=[
            pltpu.VMEM(pair_left.shape, BF16),
            pltpu.VMEM(pair_right.shape, BF16),
            pltpu.VMEM((2, nq, width, nz * width), BF16),
            pltpu.VMEM((na * 8, nq * na * 8), BF16),
            pltpu.VMEM((nz * 2, 8, 128), F32),
            pltpu.VMEM((STEPS, nz, 8, width), F32),
            pltpu.VMEM((STEPS, 2, na, 8, nz * width), BF16),
            pltpu.VMEM((na * 8, nz * width), BF16),
            pltpu.VMEM((nq, na * 8, width), F32),
            pltpu.VMEM((STEPS, na, 8, width), F32),
            pltpu.VMEM((STEPS, na, 8, width), F32),
            pltpu.VMEM((STEPS, 2, 8, bands // 2), F32),
            pltpu.VMEM((STEPS, 8, bands // 2), F32),
            pltpu.VMEM((STEPS, nz, 8, bands // 2), F32),
            pltpu.VMEM((STEPS, 2, 8, bands // 2), F32),
            pltpu.VMEM((STEPS, na, 8, 128), F32),
            pltpu.VMEM((8, bands), F32),
            pltpu.VMEM((8, bands), F32),
            pltpu.VMEM((8, bands), F32),
            pltpu.VMEM((8, 128), F32),
            pltpu.VMEM((8, nz * width), F32),
            dma((2 + 2 * nz,)),
            dma((nz * 2,)),
            dma((nz * 2,)),
            dma((STEPS, nz)),
            dma((STEPS, nz)),
            dma((STEPS, na)),
            dma((STEPS, na)),
            dma((STEPS, na)),
            dma((STEPS, na)),
            dma((STEPS, na)),
            dma((STEPS, na)),
            dma((STEPS,)),
            dma((STEPS,)),
            dma((STEPS, nz)),
            dma((STEPS, nz)),
            dma((STEPS,)),
            dma((STEPS,)),
            dma((STEPS, na)),
            dma((STEPS, na)),
        ],
        compiler_params=pltpu.CompilerParams(
            collective_id=0, has_side_effects=True, vmem_limit_bytes=60 * 1024 * 1024
        ),
    )(pack, momentum_index, pair_left, pair_right, screened)
    return last.reshape(current.shape), prior.reshape(current.shape), alphas, betas


def solution(mesh):
    kpt, pw = mesh.devices.shape
    ny = 4 if kpt % 4 == 0 else kpt
    finer = Mesh(
        mesh.devices.reshape(ny, kpt // ny, pw // 2, 2), ("kpt_0", "kpt_1", "pw_0", "pw_1")
    )
    in_specs = (
        P(KPT, PW),
        P(None, KPT, PW),
        P(None, KPT, PW),
        P(),
        P(KPT, None, PW),
        P(KPT, None, PW),
        P(KPT, PW, None),
        P(),
    )
    out_specs = (P(None, KPT, PW), P(None, KPT, PW), P(), P())
    return jax.shard_map(
        on_device, mesh=finer, in_specs=in_specs, out_specs=out_specs, check_vma=False
    )
```

```python
import functools

import jax
import jax.numpy as jnp
from jax import lax
from jax.experimental import pallas as pl
from jax.experimental.pallas import tpu as pltpu
from jax.sharding import Mesh
from jax.sharding import PartitionSpec as P

STEPS = 3
KPT = ("kpt_0", "kpt_1")
PW = ("pw_0", "pw_1")
MESH = pl.DeviceIdType.MESH
F32 = jnp.float32
BF16 = jnp.bfloat16
NT = (((1,), (1,)), ((), ()))

epsilon = 1e-06


def kernel(
    sizes, energies, current, previous, first_beta, momentum_h, left, right, screened,
    packed,
    energies_v, current_v, previous_v, first_beta_s, momentum,
    left_v, right_v, screened_v, selector,
    pk, gath, gained, images, field, field_in, half_out, half_in, direct_z, direct_c, sums,
    vec, old, levels, beta, applied_v,
    small_sem, load_sem, pk_send, pk_recv, gz_send, gz_recv, gx_send, gx_recv, fwd_send, fwd_recv,
    field_send, field_recv, pair_send, pair_recv, dz_send, dz_recv, dc_send, dc_recv,
    sums_send, sums_recv,
):
    ny, nx, nz = sizes
    na = ny * nx
    nq, width = screened.shape[0], screened.shape[1]
    bands = left.shape[1]
    half = bands // 2
    entries = momentum.shape[0] * bands
    y, x = lax.axis_index("kpt_0"), lax.axis_index("kpt_1")
    z, c = lax.axis_index("pw_0"), lax.axis_index("pw_1")
    other = 1 - c
    a = y * nx + x
    b = z * 2 + c

    def plane_peer(i):
        ty = lax.rem(y + i // nx, ny)
        tx = lax.rem(x + lax.rem(i, nx), nx)
        return ty * nx + tx, (ty, tx, z, c)

    def plane_source(i):
        ty = lax.rem(y + ny - i // nx, ny)
        tx = lax.rem(x + nx - lax.rem(i, nx), nx)
        return ty * nx + tx

    def z_peer(i):
        tz = lax.rem(z + i, nz)
        return tz, (y, x, tz, c)

    def z_near(i):
        far, odd = (i + 1) // 2, lax.rem(i, 2)
        return lax.rem(z + odd * far + (1 - odd) * (nz - far), nz)

    def pw_peer(i):
        t = lax.rem(b + i, nz * 2)
        return t, (y, x, t // 2, lax.rem(t, 2))

    partner = (y, x, z, other)

    small = [
        pltpu.make_async_copy(source, target, small_sem.at[n])
        for n, (source, target) in enumerate(
            (
                (current, current_v),
                (previous, previous_v),
                (energies, energies_v),
                (first_beta, first_beta_s),
                (momentum_h, momentum),
            )
        )
    ]
    loads = [
        pltpu.make_async_copy(right, right_v, load_sem.at[0]),
        pltpu.make_async_copy(left, left_v, load_sem.at[1]),
    ]
    for h in range(2):
        for t in range(nz):
            at = (t * 2 + h) * width
            loads.append(
                pltpu.make_async_copy(
                    screened.at[:, :, pl.ds(at, width)],
                    screened_v.at[h, t],
                    load_sem.at[2 + h * nz + t],
                )
            )
    for copy in small + loads:
        copy.start()

    barrier = pltpu.get_barrier_semaphore()

    @pl.loop(1, na)
    def _(i):
        pl.semaphore_signal(barrier, inc=1, device_id=plane_peer(i)[1], device_id_type=MESH)

    @pl.loop(1, nz * 2)
    def _(i):
        pl.semaphore_signal(barrier, inc=1, device_id=pw_peer(i)[1], device_id_type=MESH)

    for copy in small:
        copy.wait()
    blank = jnp.zeros((4, 32), F32)
    for n in range(2):
        pk[b, n * 4 : n * 4 + 4, :] = jnp.concatenate(
            [current_v[n], previous_v[n], energies_v[...], blank], axis=1
        )

    nr = na * 8
    nk = momentum.shape[0]
    row = lax.broadcasted_iota(jnp.int32, (nr, nk), 0)
    col = lax.broadcasted_iota(jnp.int32, (nr, nk), 1)
    spread = ((row // 8) * 4 + row % 4 == col).astype(F32).astype(BF16)
    index = momentum[...].astype(F32).astype(BF16)
    by_row = jnp.dot(spread, index, preferred_element_type=F32).astype(BF16)
    by_both = lax.dot_general(by_row, spread, NT, preferred_element_type=F32).astype(jnp.int32)
    r1 = lax.broadcasted_iota(jnp.int32, (nr, nr), 0)
    r2 = lax.broadcasted_iota(jnp.int32, (nr, nr), 1)
    same = (r1 // 4) % 2 == (r2 // 4) % 2
    for q in range(nq):
        hit = jnp.logical_and(by_both == a * nq + q, same)
        selector[:, q * nr : (q + 1) * nr] = jnp.where(hit, 1.0, 0.0).astype(BF16)

    pl.semaphore_wait(barrier, na - 1 + nz * 2 - 1)

    def pk_copy(i):
        t, device = pw_peer(i)
        return pltpu.make_async_remote_copy(
            pk.at[b], pk.at[b], pk_send.at[t], pk_recv.at[b], device, device_id_type=MESH
        )

    def arrived(ref, sem):
        pltpu.make_async_copy(ref, ref, sem).wait()

    @pl.loop(1, nz * 2)
    def _(i):
        pk_copy(i).start()

    @pl.loop(1, nz * 2)
    def _(i):
        t, _d = pw_peer(i)
        arrived(pk.at[t], pk_recv.at[t])

    lane = lax.broadcasted_iota(jnp.int32, (8, 128), 1)
    for j in range(bands // 128):
        for field_at, ref in ((0, vec), (1, old), (2, levels)):
            total = jnp.zeros((8, 128), F32)
            for m in range(4):
                turned = pk[4 * j + m]
                shift = (32 * (m - field_at)) % 128
                if shift:
                    turned = pltpu.roll(turned, shift, 1)
                total = total + jnp.where(lane // 32 == m, turned, 0.0)
            ref[:, j * 128 : (j + 1) * 128] = total
    upper = lax.broadcasted_iota(jnp.int32, (8, 128), 0) < 4
    beta[...] = jnp.where(upper, first_beta_s[0], first_beta_s[1])

    def own_k(n, k):
        return lax.broadcasted_iota(jnp.int32, (8, n), 0) % 4 == k

    def row_total(column):
        first = lax.broadcasted_iota(jnp.int32, (8, 1), 0) < 4
        top = jnp.sum(jnp.where(first, column, 0.0), axis=0, keepdims=True)
        low = jnp.sum(jnp.where(first, 0.0, column), axis=0, keepdims=True)
        return jnp.where(first, top, low)

    def share(cross, norm):
        some = norm > 1e-30
        return jnp.where(some, cross / jnp.where(some, norm, 1.0), 0.0)

    def to_plane(t, tz):
        @pl.loop(1, na)
        def _(i):
            pltpu.make_async_remote_copy(
                gath.at[t, c, tz, a], gath.at[t, c, tz, a], gx_send.at[t, tz], gx_recv.at[t, tz],
                plane_peer(i)[1], device_id_type=MESH,
            ).start()

    def send_density(t, values):
        high = values.astype(BF16).astype(F32)
        both = jnp.concatenate([high, values - high], axis=0).astype(BF16)
        total = jnp.zeros((8, width), F32)
        for k in range(4):
            out = jnp.dot(both, right_v[k], preferred_element_type=F32)
            total = total + jnp.where(own_k(width, k), out[0:8] + out[8:16], 0.0)
        gath[t, c, z, a] = total.astype(BF16)

        @pl.loop(1, nz)
        def _(i):
            tz = z_near(nz - i)
            pltpu.make_async_remote_copy(
                gath.at[t, c, z, a], gath.at[t, c, z, a], gz_send.at[t, tz], gz_recv.at[t, z],
                (y, x, tz, c), device_id_type=MESH,
            ).start()

        to_plane(t, z)

    def gain(t, h, tz, first):
        block = gath[t, h, tz].astype(F32).reshape(nr, width).astype(BF16)
        for q in range(nq):
            out = lax.dot_general(block, screened_v[h, tz, q], NT, preferred_element_type=F32)
            gained[q] = out if first else gained[q] + out

    def finish(t, with_images):
        @pl.loop(1, na)
        def _(i):
            ta = plane_source(i)
            arrived(sums.at[t, ta], sums_recv.at[t, ta])

        total = jnp.sum(sums[t], axis=0)
        cross_mean = total[:, 0:1] / entries
        square_mean = total[:, 1:2] / entries
        norm_mean = total[:, 2:3] / entries
        alpha = cross_mean
        mean_square = square_mean - 2.0 * alpha * cross_mean + alpha * alpha * norm_mean
        scale = jnp.sqrt(jnp.maximum(mean_square, 0.0) + epsilon)
        vector = vec[...]
        old[...] = vector
        vec[...] = (applied_v[...] - alpha * vector) / scale
        beta[...] = jnp.broadcast_to(scale, (8, 128))
        packed[2] = jnp.where(lane == t, alpha, packed[2])
        packed[3] = jnp.where(lane == t, scale, packed[3])
        if with_images:
            every = sums[t].reshape(nr, 128)
            rest = jnp.broadcast_to(alpha[None], (na, 8, 128)).reshape(nr, 128)[:, 0:1]
            rest = rest - share(every[:, 0:1], every[:, 2:3])
            inverse = jnp.broadcast_to((1.0 / scale)[None], (na, 8, 128)).reshape(nr, 128)[:, 0:1]
            for q in range(nq):
                images[q] = (gained[q] - rest * images[q]) * inverse

    packed[2] = jnp.zeros((8, 128), F32)
    packed[3] = jnp.zeros((8, 128), F32)
    loads[0].wait()
    send_density(0, vec[...])

    @pl.loop(0, STEPS)
    def _(t):
        @pl.loop(1, nz)
        def _(i):
            tz = z_near(i)
            arrived(gath.at[t, c, tz, a], gz_recv.at[t, tz])
            to_plane(t, tz)

        @pl.when(t == 0)
        def _():
            for copy in loads[2:]:
                copy.wait()

        def forward(tz):
            arrived(gath.at[t, c, tz, pl.ds(0, na - 1)], gx_recv.at[t, tz])
            pltpu.make_async_remote_copy(
                gath.at[t, c, tz], gath.at[t, c, tz], fwd_send.at[t, tz], fwd_recv.at[t, tz],
                partner, device_id_type=MESH,
            ).start()

        forward(z)
        gain(t, c, z, True)

        @pl.loop(1, nz)
        def _(i):
            tz = z_near(i)
            forward(tz)
            gain(t, c, tz, False)

        @pl.loop(0, nz)
        def _(i):
            tz = z_near(i)
            arrived(gath.at[t, other, tz], fwd_recv.at[t, tz])
            gain(t, other, tz, False)

        @pl.when(t == 0)
        def _():
            images[...] = gained[...]

        @pl.when(t > 0)
        def _():
            finish(t - 1, True)

        values = images[...].reshape(nq * nr, width)
        high = values.astype(BF16)
        low = (values - high.astype(F32)).astype(BF16)
        chosen = jnp.dot(selector[...], high, preferred_element_type=F32)
        chosen = chosen + jnp.dot(selector[...], low, preferred_element_type=F32)
        field[t] = chosen.reshape(na, 8, width)

        @pl.loop(1, na)
        def _(i):
            ta, device = plane_peer(i)
            pltpu.make_async_remote_copy(
                field.at[t, ta], field_in.at[t, a], field_send.at[t, ta], field_recv.at[t, a],
                device, device_id_type=MESH,
            ).start()

        field_in[t, a] = field[t, a]

        @pl.loop(1, na)
        def _(i):
            ta = plane_source(i)
            arrived(field_in.at[t, ta], field_recv.at[t, ta])

        potential = jnp.sum(field_in[t], axis=0).astype(BF16)

        @pl.when(t == 0)
        def _():
            loads[1].wait()

        partial = jnp.zeros((8, bands), F32)
        for k in range(4):
            out = lax.dot_general(potential, left_v[k], NT, preferred_element_type=F32)
            partial = partial + jnp.where(own_k(bands, k), out, 0.0)
        half_out[t, 0] = partial[:, :half]
        half_out[t, 1] = partial[:, half:]
        pair = pltpu.make_async_remote_copy(
            half_out.at[t, other], half_in.at[t], pair_send.at[t], pair_recv.at[t],
            partner, device_id_type=MESH,
        )
        pair.start()
        arrived(half_in.at[t], pair_recv.at[t])
        direct_z[t, z] = half_out[t, c] + half_in[t]

        @pl.loop(1, nz)
        def _(i):
            tz, device = z_peer(i)
            pltpu.make_async_remote_copy(
                direct_z.at[t, z], direct_z.at[t, z], dz_send.at[t, tz], dz_recv.at[t, z],
                device, device_id_type=MESH,
            ).start()

        @pl.loop(1, nz)
        def _(i):
            tz, _d = z_peer(i)
            arrived(direct_z.at[t, tz], dz_recv.at[t, tz])

        direct_c[t, c] = jnp.sum(direct_z[t], axis=0)
        whole = pltpu.make_async_remote_copy(
            direct_c.at[t, c], direct_c.at[t, c], dc_send.at[t], dc_recv.at[t],
            partner, device_id_type=MESH,
        )
        whole.start()
        arrived(direct_c.at[t, other], dc_recv.at[t])
        direct = jnp.concatenate([direct_c[t, 0], direct_c[t, 1]], axis=1)

        vector = vec[...]
        applied = levels[...] * vector - direct - beta[:, 0:1] * old[...]
        cross = jnp.sum(vector * applied, axis=1, keepdims=True)
        square = jnp.sum(applied * applied, axis=1, keepdims=True)
        norm = jnp.sum(vector * vector, axis=1, keepdims=True)
        cross, square, norm = row_total(cross), row_total(square), row_total(norm)
        sums[t, a] = jnp.where(lane == 0, cross, jnp.where(lane == 1, square, norm))
        applied_v[...] = applied

        @pl.when(t < STEPS - 1)
        def _():
            send_density(t + 1, applied - share(cross, norm) * vector)

        @pl.loop(1, na)
        def _(i):
            ta, device = plane_peer(i)
            pltpu.make_async_remote_copy(
                sums.at[t, a], sums.at[t, a], sums_send.at[t, ta], sums_recv.at[t, a],
                device, device_id_type=MESH,
            ).start()

    finish(STEPS - 1, False)
    group = pl.ds(pl.multiple_of((b // 4) * 128, 128), 128)
    for n, source in enumerate((vec, old)):
        packed[n] = pltpu.roll(source[:, group], lax.rem(128 - lax.rem(b, 4) * 32, 128), 1)

    def sent(ref, sem):
        pltpu.make_async_copy(ref, ref, sem).wait()

    @pl.loop(1, nz * 2)
    def _(i):
        sent(pk.at[b], pk_send.at[pw_peer(i)[0]])

    @pl.loop(0, STEPS)
    def _(t):
        @pl.loop(1, na)
        def _(i):
            ta = plane_peer(i)[0]
            sent(field.at[t, ta], field_send.at[t, ta])
            sent(sums.at[t, a], sums_send.at[t, ta])

        @pl.loop(0, nz)
        def _(tz):
            sent(gath.at[t, c, tz, pl.ds(0, na - 1)], gx_send.at[t, tz])
            sent(gath.at[t, c, tz], fwd_send.at[t, tz])

        @pl.loop(1, nz)
        def _(i):
            tz = z_peer(i)[0]
            sent(gath.at[t, c, z, a], gz_send.at[t, tz])
            sent(direct_z.at[t, z], dz_send.at[t, tz])

        sent(half_out.at[t, other], pair_send.at[t])
        sent(direct_c.at[t, c], dc_send.at[t])


def unpack(packed, last, prior, alphas, betas):
    for n, ref in ((0, last), (1, prior)):
        ref[0] = packed[n, 0:4, :32]
        ref[1] = packed[n, 4:8, :32]
    for n, ref in ((2, alphas), (3, betas)):
        ref[0:1, :] = packed[n, 0:1, :STEPS]
        ref[1:2, :] = packed[n, 4:5, :STEPS]


def on_device(
    energies, current, previous, previous_beta, pair_left, pair_right, screened, momentum_index
):
    ny, nx, nz = lax.axis_size("kpt_0"), lax.axis_size("kpt_1"), lax.axis_size("pw_0")
    na = ny * nx
    nvec = current.shape[0]
    bands, width = pair_left.shape[1:]
    nq = screened.shape[0]
    dma = pltpu.SemaphoreType.DMA
    vmem = pl.BlockSpec(memory_space=pltpu.VMEM)
    hbm = pl.BlockSpec(memory_space=pl.ANY)
    packed = pl.pallas_call(
        functools.partial(kernel, (ny, nx, nz)),
        out_shape=jax.ShapeDtypeStruct((4, 8, 128), F32),
        in_specs=[hbm] * 8,
        out_specs=vmem,
        scratch_shapes=[
            pltpu.VMEM(energies.shape, F32),
            pltpu.VMEM(current.shape, F32),
            pltpu.VMEM(previous.shape, F32),
            pltpu.SMEM(previous_beta.shape, F32),
            pltpu.VMEM(momentum_index.shape, jnp.int32),
            pltpu.VMEM(pair_left.shape, BF16),
            pltpu.VMEM(pair_right.shape, BF16),
            pltpu.VMEM((2, nz, nq, width, width), BF16),
            pltpu.VMEM((na * 8, nq * na * 8), BF16),
            pltpu.VMEM((nz * 2, 8, 128), F32),
            pltpu.VMEM((STEPS, 2, nz, na, 8, width), BF16),
            pltpu.VMEM((nq, na * 8, width), F32),
            pltpu.VMEM((nq, na * 8, width), F32),
            pltpu.VMEM((STEPS, na, 8, width), F32),
            pltpu.VMEM((STEPS, na, 8, width), F32),
            pltpu.VMEM((STEPS, 2, 8, bands // 2), F32),
            pltpu.VMEM((STEPS, 8, bands // 2), F32),
            pltpu.VMEM((STEPS, nz, 8, bands // 2), F32),
            pltpu.VMEM((STEPS, 2, 8, bands // 2), F32),
            pltpu.VMEM((STEPS, na, 8, 128), F32),
            pltpu.VMEM((8, bands), F32),
            pltpu.VMEM((8, bands), F32),
            pltpu.VMEM((8, bands), F32),
            pltpu.VMEM((8, 128), F32),
            pltpu.VMEM((8, bands), F32),
            dma((5,)),
            dma((2 + 2 * nz,)),
            dma((nz * 2,)),
            dma((nz * 2,)),
            dma((STEPS, nz)),
            dma((STEPS, nz)),
            dma((STEPS, nz)),
            dma((STEPS, nz)),
            dma((STEPS, nz)),
            dma((STEPS, nz)),
            dma((STEPS, na)),
            dma((STEPS, na)),
            dma((STEPS,)),
            dma((STEPS,)),
            dma((STEPS, nz)),
            dma((STEPS, nz)),
            dma((STEPS,)),
            dma((STEPS,)),
            dma((STEPS, na)),
            dma((STEPS, na)),
        ],
        compiler_params=pltpu.CompilerParams(
            collective_id=0, has_side_effects=True, vmem_limit_bytes=60 * 1024 * 1024
        ),
    )(
        energies, current, previous, previous_beta, momentum_index, pair_left, pair_right, screened
    )
    return tuple(
        pl.pallas_call(
            unpack,
            out_shape=(
                jax.ShapeDtypeStruct(current.shape, F32),
                jax.ShapeDtypeStruct(current.shape, F32),
                jax.ShapeDtypeStruct((nvec, STEPS), F32),
                jax.ShapeDtypeStruct((nvec, STEPS), F32),
            ),
            in_specs=[vmem],
            out_specs=(vmem, vmem, vmem, vmem),
        )(packed)
    )


def solution(mesh):
    kpt, pw = mesh.devices.shape
    ny = 4 if kpt % 4 == 0 else kpt
    finer = Mesh(
        mesh.devices.reshape(ny, kpt // ny, pw // 2, 2), ("kpt_0", "kpt_1", "pw_0", "pw_1")
    )
    in_specs = (
        P(KPT, PW),
        P(None, KPT, PW),
        P(None, KPT, PW),
        P(),
        P(KPT, None, PW),
        P(KPT, None, PW),
        P(KPT, PW, None),
        P(),
    )
    out_specs = (P(None, KPT, PW), P(None, KPT, PW), P(), P())
    return jax.shard_map(
        on_device, mesh=finer, in_specs=in_specs, out_specs=out_specs, check_vma=False
    )
```

```python
import functools

import jax
import jax.numpy as jnp
from jax import lax
from jax.experimental import pallas as pl
from jax.experimental.pallas import tpu as pltpu
from jax.sharding import Mesh
from jax.sharding import PartitionSpec as P

STEPS = 3
KPT = ("kpt_0", "kpt_1")
PW = ("pw_0", "pw_1")
MESH = pl.DeviceIdType.MESH
F32 = jnp.float32
BF16 = jnp.bfloat16
NT = (((1,), (1,)), ((), ()))

epsilon = 1e-06


def kernel(
    sizes, energies, current, previous, first_beta, momentum_h, left, right, screened,
    packed,
    energies_v, current_v, previous_v, first_beta_s, momentum,
    left_v, right_v, screened_v, selector,
    left_o, pk, gath, gained, images, field, field_in, direct, sums,
    vec, old, levels, beta, applied_v, rest_v, inverse_v,
    small_sem, load_sem, pk_send, pk_recv, gz_send, gz_recv, gx_send, gx_recv, fwd_send, fwd_recv,
    field_send, field_recv, direct_send, direct_recv, sums_send, sums_recv, left_send, left_recv,
):
    ny, nx, nz = sizes
    na = ny * nx
    nq, width = screened.shape[0], screened.shape[1]
    bands = left.shape[1]
    half = bands // 2
    entries = momentum.shape[0] * bands
    y, x = lax.axis_index("kpt_0"), lax.axis_index("kpt_1")
    z, c = lax.axis_index("pw_0"), lax.axis_index("pw_1")
    other = 1 - c
    a = y * nx + x
    b = z * 2 + c

    tys = [lax.rem(y + d, ny) for d in range(ny)]
    txs = [lax.rem(x + d, nx) for d in range(nx)]
    far_first = sorted(
        ((dy, dx) for dy in range(ny) for dx in range(nx) if dy or dx),
        key=lambda d: -min(d[0], ny - d[0]) - min(d[1], nx - d[1]),
    )

    def plane_sends(send):
        for dy, dx in far_first:
            send(tys[dy] * nx + txs[dx], tys[dy], txs[dx])

    def plane_source(i):
        ty = lax.rem(y + ny - i // nx, ny)
        tx = lax.rem(x + nx - lax.rem(i, nx), nx)
        return ty * nx + tx

    def z_peer(i):
        tz = lax.rem(z + i, nz)
        return tz, (y, x, tz, c)

    def z_near(i):
        far, odd = (i + 1) // 2, lax.rem(i, 2)
        return lax.rem(z + odd * far + (1 - odd) * (nz - far), nz)

    def pw_peer(i):
        t = lax.rem(b + i, nz * 2)
        return t, (y, x, t // 2, lax.rem(t, 2))

    partner = (y, x, z, other)

    small = [
        pltpu.make_async_copy(source, target, small_sem.at[n])
        for n, (source, target) in enumerate(
            (
                (current, current_v),
                (previous, previous_v),
                (energies, energies_v),
                (first_beta, first_beta_s),
                (momentum_h, momentum),
            )
        )
    ]
    loads = [
        pltpu.make_async_copy(right, right_v, load_sem.at[0]),
        pltpu.make_async_copy(left, left_v, load_sem.at[1]),
    ]
    for h in range(2):
        for t in range(nz):
            at = (t * 2 + h) * width
            loads.append(
                pltpu.make_async_copy(
                    screened.at[:, :, pl.ds(at, width)],
                    screened_v.at[h, t],
                    load_sem.at[2 + h * nz + t],
                )
            )
    for copy in small + loads:
        copy.start()

    barrier = pltpu.get_barrier_semaphore()

    def greet(device):
        pl.semaphore_signal(barrier, inc=1, device_id=device, device_id_type=MESH)

    @pl.loop(1, nz * 2)
    def _(i):
        greet(pw_peer(i)[1])

    def greet_both(ta, ty, tx):
        greet((ty, tx, z, c))
        greet((ty, tx, z, other))

    plane_sends(greet_both)

    for copy in small:
        copy.wait()
    blank = jnp.zeros((4, 32), F32)
    for n in range(2):
        pk[b, n * 4 : n * 4 + 4, :] = jnp.concatenate(
            [current_v[n], previous_v[n], energies_v[...], blank], axis=1
        )

    nr = na * 8
    nk = momentum.shape[0]
    row = lax.broadcasted_iota(jnp.int32, (nr, nk), 0)
    col = lax.broadcasted_iota(jnp.int32, (nr, nk), 1)
    spread = ((row // 8) * 4 + row % 4 == col).astype(F32).astype(BF16)
    index = momentum[...].astype(F32).astype(BF16)
    by_row = jnp.dot(spread, index, preferred_element_type=F32).astype(BF16)
    by_both = lax.dot_general(by_row, spread, NT, preferred_element_type=F32).astype(jnp.int32)
    r1 = lax.broadcasted_iota(jnp.int32, (nr, nr), 0)
    r2 = lax.broadcasted_iota(jnp.int32, (nr, nr), 1)
    same = (r1 // 4) % 2 == (r2 // 4) % 2
    for q in range(nq):
        hit = jnp.logical_and(by_both == a * nq + q, same)
        selector[:, q * nr : (q + 1) * nr] = jnp.where(hit, 1.0, 0.0).astype(BF16)

    pl.semaphore_wait(barrier, 2 * (na - 1) + nz * 2 - 1)

    left_copy = pltpu.make_async_remote_copy(
        left_v.at[:, pl.ds(pl.multiple_of(other * half, half), half), :], left_o,
        left_send, left_recv, partner, device_id_type=MESH,
    )

    def pk_copy(i):
        t, device = pw_peer(i)
        return pltpu.make_async_remote_copy(
            pk.at[b], pk.at[b], pk_send.at[t], pk_recv.at[b], device, device_id_type=MESH
        )

    def arrived(ref, sem):
        pltpu.make_async_copy(ref, ref, sem).wait()

    @pl.loop(1, nz * 2)
    def _(i):
        pk_copy(i).start()

    @pl.loop(1, nz * 2)
    def _(i):
        t, _d = pw_peer(i)
        arrived(pk.at[t], pk_recv.at[t])

    lane = lax.broadcasted_iota(jnp.int32, (8, 128), 1)
    for j in range(bands // 128):
        for field_at, ref in ((0, vec), (1, old), (2, levels)):
            total = jnp.zeros((8, 128), F32)
            for m in range(4):
                turned = pk[4 * j + m]
                shift = (32 * (m - field_at)) % 128
                if shift:
                    turned = pltpu.roll(turned, shift, 1)
                total = total + jnp.where(lane // 32 == m, turned, 0.0)
            ref[:, j * 128 : (j + 1) * 128] = total
    upper = lax.broadcasted_iota(jnp.int32, (8, 128), 0) < 4
    beta[...] = jnp.where(upper, first_beta_s[0], first_beta_s[1])

    def own_k(n, k):
        return lax.broadcasted_iota(jnp.int32, (8, n), 0) % 4 == k

    def row_total(column):
        first = lax.broadcasted_iota(jnp.int32, (8, 1), 0) < 4
        top = jnp.sum(jnp.where(first, column, 0.0), axis=0, keepdims=True)
        low = jnp.sum(jnp.where(first, 0.0, column), axis=0, keepdims=True)
        return jnp.where(first, top, low)

    def share(cross, norm):
        some = norm > 1e-30
        return jnp.where(some, cross / jnp.where(some, norm, 1.0), 0.0)

    def to_plane(t, tz):
        def send(ta, ty, tx):
            pltpu.make_async_remote_copy(
                gath.at[t, c, tz, a], gath.at[t, c, tz, a], gx_send.at[t, tz], gx_recv.at[t, tz],
                (ty, tx, z, c), device_id_type=MESH,
            ).start()

        plane_sends(send)

    def send_density(t, values):
        high = values.astype(BF16).astype(F32)
        both = jnp.concatenate([high, values - high], axis=0).astype(BF16)
        total = jnp.zeros((8, width), F32)
        for k in range(4):
            out = jnp.dot(both, right_v[k], preferred_element_type=F32)
            total = total + jnp.where(own_k(width, k), out[0:8] + out[8:16], 0.0)
        gath[t, c, z, a] = total.astype(BF16)

        @pl.loop(1, nz)
        def _(i):
            tz = z_near(nz - i)
            pltpu.make_async_remote_copy(
                gath.at[t, c, z, a], gath.at[t, c, z, a], gz_send.at[t, tz], gz_recv.at[t, z],
                (y, x, tz, c), device_id_type=MESH,
            ).start()

        to_plane(t, z)

    def gain(t, h, tz, first):
        block = gath[t, h, tz].astype(F32).reshape(nr, width).astype(BF16)
        for q in range(nq):
            out = lax.dot_general(block, screened_v[h, tz, q], NT, preferred_element_type=F32)
            gained[q] = out if first else gained[q] + out

    def finish(t):
        arrived(sums.at[t, pl.ds(0, na - 1)], sums_recv.at[t])
        total = jnp.sum(sums[t], axis=0)
        cross_mean = total[:, 0:1] / entries
        square_mean = total[:, 1:2] / entries
        norm_mean = total[:, 2:3] / entries
        alpha = cross_mean
        mean_square = square_mean - 2.0 * alpha * cross_mean + alpha * alpha * norm_mean
        scale = jnp.sqrt(jnp.maximum(mean_square, 0.0) + epsilon)
        vector = vec[...]
        old[...] = vector
        vec[...] = (applied_v[...] - alpha * vector) / scale
        beta[...] = jnp.broadcast_to(scale, (8, 128))
        packed[2] = jnp.where(lane == t, alpha, packed[2])
        packed[3] = jnp.where(lane == t, scale, packed[3])
        every = sums[t].reshape(nr, 128)
        rest = jnp.broadcast_to(alpha[None], (na, 8, 128)).reshape(nr, 128)
        rest_v[...] = rest - share(every[:, 0:1], every[:, 2:3])
        inverse_v[...] = jnp.broadcast_to((1.0 / scale)[None], (na, 8, 128)).reshape(nr, 128)

    packed[2] = jnp.zeros((8, 128), F32)
    packed[3] = jnp.zeros((8, 128), F32)
    rest_v[...] = jnp.zeros_like(rest_v)
    inverse_v[...] = jnp.ones_like(inverse_v)
    images[...] = jnp.zeros_like(images)
    loads[0].wait()
    send_density(0, vec[...])
    loads[1].wait()
    left_copy.start()

    @pl.loop(0, STEPS)
    def _(t):
        @pl.loop(1, nz)
        def _(i):
            tz = z_near(i)
            arrived(gath.at[t, c, tz, a], gz_recv.at[t, tz])
            to_plane(t, tz)

        @pl.when(t == 0)
        def _():
            for copy in loads[2:]:
                copy.wait()

        def forward(tz):
            arrived(gath.at[t, c, tz, pl.ds(0, na - 1)], gx_recv.at[t, tz])
            pltpu.make_async_remote_copy(
                gath.at[t, c, tz], gath.at[t, c, tz], fwd_send.at[t, tz], fwd_recv.at[t, tz],
                partner, device_id_type=MESH,
            ).start()

        forward(z)
        gain(t, c, z, True)

        @pl.loop(1, nz)
        def _(i):
            tz = z_near(i)
            forward(tz)
            gain(t, c, tz, False)

        @pl.when(t > 0)
        def _():
            finish(t - 1)

        @pl.loop(0, nz)
        def _(i):
            tz = z_near(i)
            arrived(gath.at[t, other, tz], fwd_recv.at[t, tz])
            gain(t, other, tz, False)

        rest, inverse = rest_v[:, 0:1], inverse_v[:, 0:1]
        for q in range(nq):
            images[q] = (gained[q] - rest * images[q]) * inverse

        values = images[...].reshape(nq * nr, width)
        high = values.astype(BF16)
        low = (values - high.astype(F32)).astype(BF16)
        chosen = jnp.dot(selector[...], high, preferred_element_type=F32)
        chosen = chosen + jnp.dot(selector[...], low, preferred_element_type=F32)
        field[t] = chosen.reshape(na, 8, width).astype(BF16)

        def send_field(ta, ty, tx):
            for n, core in enumerate((c, other)):
                pltpu.make_async_remote_copy(
                    field.at[t, ta], field_in.at[t, c, a], field_send.at[t, n],
                    field_recv.at[t, c], (ty, tx, z, core), device_id_type=MESH,
                ).start()

        plane_sends(send_field)
        pltpu.make_async_remote_copy(
            field.at[t, a], field_in.at[t, c, a], field_send.at[t, 1],
            field_recv.at[t, c], partner, device_id_type=MESH,
        ).start()
        field_in[t, c, a] = field[t, a]

        @pl.when(t == 0)
        def _():
            left_copy.wait()

        def two_terms(values):
            high = values.astype(BF16).astype(F32)
            return jnp.concatenate([high, values - high], axis=0).astype(BF16)

        arrived(field_in.at[t, c, pl.ds(0, na - 1)], field_recv.at[t, c])
        mine = two_terms(jnp.sum(field_in[t, c].astype(F32), axis=0))
        arrived(field_in.at[t, other], field_recv.at[t, other])
        theirs = two_terms(jnp.sum(field_in[t, other].astype(F32), axis=0))
        partial = jnp.zeros((8, half), F32)
        bands_at = pl.ds(pl.multiple_of(c * half, half), half)
        for k in range(4):
            out = lax.dot_general(mine, left_v[k, bands_at, :], NT, preferred_element_type=F32)
            out += lax.dot_general(theirs, left_o[k], NT, preferred_element_type=F32)
            partial = partial + jnp.where(own_k(half, k), out[0:8] + out[8:16], 0.0)
        direct[t, c, z] = partial.astype(BF16)

        @pl.loop(1, nz)
        def _(i):
            tz = z_near(nz - i)
            for n, core in enumerate((c, other)):
                pltpu.make_async_remote_copy(
                    direct.at[t, c, z], direct.at[t, c, z], direct_send.at[t, n],
                    direct_recv.at[t, c], (y, x, tz, core), device_id_type=MESH,
                ).start()

        pltpu.make_async_remote_copy(
            direct.at[t, c, z], direct.at[t, c, z], direct_send.at[t, 1],
            direct_recv.at[t, c], partner, device_id_type=MESH,
        ).start()
        arrived(direct.at[t, c, pl.ds(0, nz - 1)], direct_recv.at[t, c])
        arrived(direct.at[t, other], direct_recv.at[t, other])
        whole = jnp.concatenate(
            [jnp.sum(direct[t, h].astype(F32), axis=0) for h in range(2)], axis=1
        )

        vector = vec[...]
        applied = levels[...] * vector - whole - beta[:, 0:1] * old[...]
        cross = jnp.sum(vector * applied, axis=1, keepdims=True)
        square = jnp.sum(applied * applied, axis=1, keepdims=True)
        norm = jnp.sum(vector * vector, axis=1, keepdims=True)
        cross, square, norm = row_total(cross), row_total(square), row_total(norm)
        sums[t, a] = jnp.where(lane == 0, cross, jnp.where(lane == 1, square, norm))
        applied_v[...] = applied

        @pl.when(t < STEPS - 1)
        def _():
            send_density(t + 1, applied - share(cross, norm) * vector)

        def send_sums(ta, ty, tx):
            pltpu.make_async_remote_copy(
                sums.at[t, a], sums.at[t, a], sums_send.at[t], sums_recv.at[t],
                (ty, tx, z, c), device_id_type=MESH,
            ).start()

        plane_sends(send_sums)

    finish(STEPS - 1)
    group = pl.ds(pl.multiple_of((b // 4) * 128, 128), 128)
    for n, source in enumerate((vec, old)):
        packed[n] = pltpu.roll(source[:, group], lax.rem(128 - lax.rem(b, 4) * 32, 128), 1)

    def sent(ref, sem):
        pltpu.make_async_copy(ref, ref, sem).wait()

    @pl.loop(1, nz * 2)
    def _(i):
        sent(pk.at[b], pk_send.at[pw_peer(i)[0]])

    @pl.loop(0, STEPS)
    def _(t):
        sent(field.at[t, pl.ds(0, na - 1)], field_send.at[t, 0])
        sent(field.at[t], field_send.at[t, 1])
        sent(sums.at[t, pl.ds(0, na - 1)], sums_send.at[t])
        sent(direct.at[t, c, pl.ds(0, nz - 1)], direct_send.at[t, 0])
        sent(direct.at[t, c], direct_send.at[t, 1])

        @pl.loop(0, nz)
        def _(tz):
            sent(gath.at[t, c, tz, pl.ds(0, na - 1)], gx_send.at[t, tz])
            sent(gath.at[t, c, tz], fwd_send.at[t, tz])

        @pl.loop(1, nz)
        def _(i):
            tz = z_peer(i)[0]
            sent(gath.at[t, c, z, a], gz_send.at[t, tz])


def unpack(packed, last, prior, alphas, betas):
    for n, ref in ((0, last), (1, prior)):
        ref[0] = packed[n, 0:4, :32]
        ref[1] = packed[n, 4:8, :32]
    for n, ref in ((2, alphas), (3, betas)):
        ref[0:1, :] = packed[n, 0:1, :STEPS]
        ref[1:2, :] = packed[n, 4:5, :STEPS]


def on_device(
    energies, current, previous, previous_beta, pair_left, pair_right, screened, momentum_index
):
    ny, nx, nz = lax.axis_size("kpt_0"), lax.axis_size("kpt_1"), lax.axis_size("pw_0")
    na = ny * nx
    nvec = current.shape[0]
    bands, width = pair_left.shape[1:]
    nq = screened.shape[0]
    dma = pltpu.SemaphoreType.DMA
    vmem = pl.BlockSpec(memory_space=pltpu.VMEM)
    hbm = pl.BlockSpec(memory_space=pl.ANY)
    packed = pl.pallas_call(
        functools.partial(kernel, (ny, nx, nz)),
        out_shape=jax.ShapeDtypeStruct((4, 8, 128), F32),
        in_specs=[hbm] * 8,
        out_specs=vmem,
        scratch_shapes=[
            pltpu.VMEM(energies.shape, F32),
            pltpu.VMEM(current.shape, F32),
            pltpu.VMEM(previous.shape, F32),
            pltpu.SMEM(previous_beta.shape, F32),
            pltpu.VMEM(momentum_index.shape, jnp.int32),
            pltpu.VMEM(pair_left.shape, BF16),
            pltpu.VMEM(pair_right.shape, BF16),
            pltpu.VMEM((2, nz, nq, width, width), BF16),
            pltpu.VMEM((na * 8, nq * na * 8), BF16),
            pltpu.VMEM((4, bands // 2, width), BF16),
            pltpu.VMEM((nz * 2, 8, 128), F32),
            pltpu.VMEM((STEPS, 2, nz, na, 8, width), BF16),
            pltpu.VMEM((nq, na * 8, width), F32),
            pltpu.VMEM((nq, na * 8, width), F32),
            pltpu.VMEM((STEPS, na, 8, width), BF16),
            pltpu.VMEM((STEPS, 2, na, 8, width), BF16),
            pltpu.VMEM((STEPS, 2, nz, 8, bands // 2), BF16),
            pltpu.VMEM((STEPS, na, 8, 128), F32),
            pltpu.VMEM((8, bands), F32),
            pltpu.VMEM((8, bands), F32),
            pltpu.VMEM((8, bands), F32),
            pltpu.VMEM((8, 128), F32),
            pltpu.VMEM((8, bands), F32),
            pltpu.VMEM((na * 8, 128), F32),
            pltpu.VMEM((na * 8, 128), F32),
            dma((5,)),
            dma((2 + 2 * nz,)),
            dma((nz * 2,)),
            dma((nz * 2,)),
            dma((STEPS, nz)),
            dma((STEPS, nz)),
            dma((STEPS, nz)),
            dma((STEPS, nz)),
            dma((STEPS, nz)),
            dma((STEPS, nz)),
            dma((STEPS, 2)),
            dma((STEPS, 2)),
            dma((STEPS, 2)),
            dma((STEPS, 2)),
            dma((STEPS,)),
            dma((STEPS,)),
            dma(()),
            dma(()),
        ],
        compiler_params=pltpu.CompilerParams(
            collective_id=0, has_side_effects=True, vmem_limit_bytes=60 * 1024 * 1024
        ),
    )(
        energies, current, previous, previous_beta, momentum_index, pair_left, pair_right, screened
    )
    return tuple(
        pl.pallas_call(
            unpack,
            out_shape=(
                jax.ShapeDtypeStruct(current.shape, F32),
                jax.ShapeDtypeStruct(current.shape, F32),
                jax.ShapeDtypeStruct((nvec, STEPS), F32),
                jax.ShapeDtypeStruct((nvec, STEPS), F32),
            ),
            in_specs=[vmem],
            out_specs=(vmem, vmem, vmem, vmem),
        )(packed)
    )


def solution(mesh):
    kpt, pw = mesh.devices.shape
    ny = 4 if kpt % 4 == 0 else kpt
    finer = Mesh(
        mesh.devices.reshape(ny, kpt // ny, pw // 2, 2), ("kpt_0", "kpt_1", "pw_0", "pw_1")
    )
    in_specs = (
        P(KPT, PW),
        P(None, KPT, PW),
        P(None, KPT, PW),
        P(),
        P(KPT, None, PW),
        P(KPT, None, PW),
        P(KPT, PW, None),
        P(),
    )
    out_specs = (P(None, KPT, PW), P(None, KPT, PW), P(), P())
    return jax.shard_map(
        on_device, mesh=finer, in_specs=in_specs, out_specs=out_specs, check_vma=False
    )
```

```python
import functools

import jax
import jax.numpy as jnp
from jax import lax
from jax.experimental import pallas as pl
from jax.experimental.pallas import tpu as pltpu
from jax.sharding import Mesh
from jax.sharding import PartitionSpec as P

STEPS = 3
NEAR = 1
KPT = ("kpt_0", "kpt_1")
PW = ("pw_0", "pw_1")
MESH = pl.DeviceIdType.MESH
F32 = jnp.float32
BF16 = jnp.bfloat16
NT = (((1,), (1,)), ((), ()))

epsilon = 1e-06


def kernel(
    sizes, energies, current, previous, first_beta, momentum_h, left, right, screened,
    packed,
    energies_v, current_v, previous_v, first_beta_s, momentum,
    left_v, right_v, screened_v, selector,
    left_o, pk, gath, gained, images, field, field_in, direct, sums,
    vec, old, levels, beta, applied_v, rest_v, inverse_v,
    small_sem, load_sem, pk_send, pk_recv, gz_send, gz_recv, gx_send, gx_recv, fwd_send, fwd_recv,
    field_send, field_recv, direct_send, direct_recv, sums_send, sums_recv, left_send, left_recv,
):
    ny, nx, nz = sizes
    na = ny * nx
    nq, width = screened.shape[0], screened.shape[1]
    bands = left.shape[1]
    half = bands // 2
    entries = momentum.shape[0] * bands
    y, x = lax.axis_index("kpt_0"), lax.axis_index("kpt_1")
    z, c = lax.axis_index("pw_0"), lax.axis_index("pw_1")
    other = 1 - c
    a = y * nx + x
    b = z * 2 + c

    tys = [lax.rem(y + d, ny) for d in range(ny)]
    txs = [lax.rem(x + d, nx) for d in range(nx)]
    far_first = sorted(
        ((dy, dx) for dy in range(ny) for dx in range(nx) if dy or dx),
        key=lambda d: -min(d[0], ny - d[0]) - min(d[1], nx - d[1]),
    )

    def plane_sends(send):
        for dy, dx in far_first:
            send(tys[dy] * nx + txs[dx], tys[dy], txs[dx])

    def plane_source(i):
        ty = lax.rem(y + ny - i // nx, ny)
        tx = lax.rem(x + nx - lax.rem(i, nx), nx)
        return ty * nx + tx

    def z_near(i):
        far, odd = (i + 1) // 2, lax.rem(i, 2)
        return lax.rem(z + odd * far + (1 - odd) * (nz - far), nz)

    partner = (y, x, z, other)

    small = [
        pltpu.make_async_copy(source, target, small_sem.at[n])
        for n, (source, target) in enumerate(
            (
                (current, current_v),
                (previous, previous_v),
                (energies, energies_v),
                (first_beta, first_beta_s),
                (momentum_h, momentum),
            )
        )
    ]
    loads = [
        pltpu.make_async_copy(right, right_v, load_sem.at[0]),
        pltpu.make_async_copy(left, left_v, load_sem.at[1]),
    ]
    for h in range(2):
        for t in range(nz):
            at = (t * 2 + h) * width
            loads.append(
                pltpu.make_async_copy(
                    screened.at[:, :, pl.ds(at, width)],
                    screened_v.at[h, t],
                    load_sem.at[2 + h * nz + t],
                )
            )
    for copy in small + loads:
        copy.start()

    barrier = pltpu.get_barrier_semaphore()

    def greet(device):
        pl.semaphore_signal(barrier, inc=1, device_id=device, device_id_type=MESH)

    @pl.loop(1, nz)
    def _(i):
        tz = z_near(nz - i)
        greet((y, x, tz, c))
        greet((y, x, tz, other))

    def greet_both(ta, ty, tx):
        greet((ty, tx, z, c))
        greet((ty, tx, z, other))

    plane_sends(greet_both)
    greet(partner)

    for copy in small:
        copy.wait()
    blank = jnp.zeros((4, 32), F32)
    for n in range(2):
        pk[b, n * 4 : n * 4 + 4, :] = jnp.concatenate(
            [current_v[n], previous_v[n], energies_v[...], blank], axis=1
        )

    nr = na * 8
    nk = momentum.shape[0]
    row = lax.broadcasted_iota(jnp.int32, (nr, nk), 0)
    col = lax.broadcasted_iota(jnp.int32, (nr, nk), 1)
    spread = ((row // 8) * 4 + row % 4 == col).astype(F32).astype(BF16)
    index = momentum[...].astype(F32).astype(BF16)
    by_row = jnp.dot(spread, index, preferred_element_type=F32).astype(BF16)
    by_both = lax.dot_general(by_row, spread, NT, preferred_element_type=F32).astype(jnp.int32)
    r1 = lax.broadcasted_iota(jnp.int32, (nr, nr), 0)
    r2 = lax.broadcasted_iota(jnp.int32, (nr, nr), 1)
    same = (r1 // 4) % 2 == (r2 // 4) % 2
    for q in range(nq):
        hit = jnp.logical_and(by_both == a * nq + q, same)
        selector[:, q * nr : (q + 1) * nr] = jnp.where(hit, 1.0, 0.0).astype(BF16)

    pl.semaphore_wait(barrier, 2 * (na - 1) + nz * 2 - 1)

    left_copy = pltpu.make_async_remote_copy(
        left_v.at[:, pl.ds(pl.multiple_of(other * half, half), half), :], left_o,
        left_send, left_recv, partner, device_id_type=MESH,
    )

    def arrived(ref, sem):
        pltpu.make_async_copy(ref, ref, sem).wait()

    def send_pk(n, device):
        pltpu.make_async_remote_copy(
            pk.at[b], pk.at[b], pk_send.at[n], pk_recv.at[0], device, device_id_type=MESH
        ).start()

    @pl.loop(1, nz)
    def _(i):
        tz = z_near(nz - i)
        send_pk(0, (y, x, tz, c))
        send_pk(0, (y, x, tz, other))

    send_pk(0, partner)
    arrived(pk.at[pl.ds(0, nz * 2 - 1)], pk_recv.at[0])

    lane = lax.broadcasted_iota(jnp.int32, (8, 128), 1)
    for j in range(bands // 128):
        for field_at, ref in ((0, vec), (1, old), (2, levels)):
            total = jnp.zeros((8, 128), F32)
            for m in range(4):
                turned = pk[4 * j + m]
                shift = (32 * (m - field_at)) % 128
                if shift:
                    turned = pltpu.roll(turned, shift, 1)
                total = total + jnp.where(lane // 32 == m, turned, 0.0)
            ref[:, j * 128 : (j + 1) * 128] = total
    upper = lax.broadcasted_iota(jnp.int32, (8, 128), 0) < 4
    beta[...] = jnp.where(upper, first_beta_s[0], first_beta_s[1])

    def own_k(n, k):
        return lax.broadcasted_iota(jnp.int32, (8, n), 0) % 4 == k

    def row_total(column):
        first = lax.broadcasted_iota(jnp.int32, (8, 1), 0) < 4
        top = jnp.sum(jnp.where(first, column, 0.0), axis=0, keepdims=True)
        low = jnp.sum(jnp.where(first, 0.0, column), axis=0, keepdims=True)
        return jnp.where(first, top, low)

    def share(cross, norm):
        some = norm > 1e-30
        return jnp.where(some, cross / jnp.where(some, norm, 1.0), 0.0)

    def to_plane(t, tz):
        def send(ta, ty, tx):
            pltpu.make_async_remote_copy(
                gath.at[t, c, tz, a], gath.at[t, c, tz, a], gx_send.at[t, tz], gx_recv.at[t, tz],
                (ty, tx, z, c), device_id_type=MESH,
            ).start()

        plane_sends(send)

    def send_density(t, values):
        high = values.astype(BF16).astype(F32)
        both = jnp.concatenate([high, values - high], axis=0).astype(BF16)
        total = jnp.zeros((8, width), F32)
        for k in range(4):
            out = jnp.dot(both, right_v[k], preferred_element_type=F32)
            total = total + jnp.where(own_k(width, k), out[0:8] + out[8:16], 0.0)
        gath[t, c, z, a] = total.astype(BF16)

        @pl.loop(1, nz - 2 * NEAR)
        def _(i):
            tz = z_near(nz - i)
            pltpu.make_async_remote_copy(
                gath.at[t, c, z, a], gath.at[t, c, z, a], gz_send.at[t, tz], gz_recv.at[t, z],
                (y, x, tz, c), device_id_type=MESH,
            ).start()

        to_plane(t, z)

    def gain(t, h, tz, first):
        block = gath[t, h, tz].astype(F32).reshape(nr, width).astype(BF16)
        for q in range(nq):
            out = lax.dot_general(block, screened_v[h, tz, q], NT, preferred_element_type=F32)
            gained[q] = out if first else gained[q] + out

    def finish(t):
        arrived(sums.at[t, pl.ds(0, na - 1)], sums_recv.at[t])
        def by_row(lines, at):
            first = lax.broadcasted_iota(jnp.int32, (*lines.shape[:-2], 8, 1), lines.ndim - 2) < 4
            return jnp.where(first, lines[..., at : at + 1], lines[..., at + 3 : at + 4])

        total = jnp.sum(sums[t], axis=0)
        cross_mean = by_row(total, 0) / entries
        square_mean = by_row(total, 1) / entries
        norm_mean = by_row(total, 2) / entries
        alpha = cross_mean
        mean_square = square_mean - 2.0 * alpha * cross_mean + alpha * alpha * norm_mean
        scale = jnp.sqrt(jnp.maximum(mean_square, 0.0) + epsilon)
        vector = vec[...]
        old[...] = vector
        vec[...] = (applied_v[...] - alpha * vector) / scale
        beta[...] = jnp.broadcast_to(scale, (8, 128))
        packed[2] = jnp.where(lane == t, alpha, packed[2])
        packed[3] = jnp.where(lane == t, scale, packed[3])
        every = sums[t]
        shares = share(by_row(every, 0), by_row(every, 2))
        rest_v[...] = jnp.broadcast_to(alpha[None] - shares, (na, 8, 128)).reshape(nr, 128)
        inverse_v[...] = jnp.broadcast_to((1.0 / scale)[None], (na, 8, 128)).reshape(nr, 128)

    packed[2] = jnp.zeros((8, 128), F32)
    packed[3] = jnp.zeros((8, 128), F32)
    rest_v[...] = jnp.zeros_like(rest_v)
    inverse_v[...] = jnp.ones_like(inverse_v)
    loads[0].wait()
    send_density(0, vec[...])
    loads[1].wait()
    left_copy.start()

    @pl.loop(0, STEPS)
    def _(t):
        @pl.loop(1 + 2 * NEAR, nz)
        def _(i):
            tz = z_near(i)
            arrived(gath.at[t, c, tz, a], gz_recv.at[t, tz])
            to_plane(t, tz)

        @pl.when(t == 0)
        def _():
            for copy in loads[2:]:
                copy.wait()

        def forward(tz):
            pltpu.make_async_remote_copy(
                gath.at[t, c, tz], gath.at[t, c, tz], fwd_send.at[t, tz], fwd_recv.at[t, tz],
                partner, device_id_type=MESH,
            ).start()

        arrived(gath.at[t, c, z, pl.ds(0, na - 1)], gx_recv.at[t, z])

        @pl.loop(1, 1 + 2 * NEAR)
        def _(i):
            tz = z_near(i)
            pltpu.make_async_remote_copy(
                gath.at[t, c, z], gath.at[t, c, z], gz_send.at[t, tz], gz_recv.at[t, z],
                (y, x, tz, c), device_id_type=MESH,
            ).start()

        forward(z)
        gain(t, c, z, True)

        @pl.loop(1, 1 + 2 * NEAR)
        def _(i):
            tz = z_near(i)
            arrived(gath.at[t, c, tz], gz_recv.at[t, tz])
            forward(tz)
            gain(t, c, tz, False)

        @pl.loop(1 + 2 * NEAR, nz)
        def _(i):
            tz = z_near(i)
            arrived(gath.at[t, c, tz, pl.ds(0, na - 1)], gx_recv.at[t, tz])
            forward(tz)
            gain(t, c, tz, False)

        @pl.when(t > 0)
        def _():
            finish(t - 1)
            for q in range(nq):
                gained[q] = gained[q] - rest_v[:, 0:1] * images[q]

        @pl.loop(0, nz)
        def _(i):
            tz = z_near(i)
            arrived(gath.at[t, other, tz], fwd_recv.at[t, tz])
            gain(t, other, tz, False)


        values = gained[...].reshape(nq * nr, width)
        high = values.astype(BF16)
        low = (values - high.astype(F32)).astype(BF16)
        chosen = jnp.dot(selector[...], high, preferred_element_type=F32)
        chosen = chosen + jnp.dot(selector[...], low, preferred_element_type=F32)
        inverse = inverse_v[:, 0:1]
        field[t] = (chosen * inverse).reshape(na, 8, width).astype(BF16)

        def send_field(ta, ty, tx):
            for n, core in enumerate((c, other)):
                pltpu.make_async_remote_copy(
                    field.at[t, ta], field_in.at[t, c, a], field_send.at[t, n],
                    field_recv.at[t, c], (ty, tx, z, core), device_id_type=MESH,
                ).start()

        plane_sends(send_field)
        pltpu.make_async_remote_copy(
            field.at[t, a], field_in.at[t, c, a], field_send.at[t, 1],
            field_recv.at[t, c], partner, device_id_type=MESH,
        ).start()
        field_in[t, c, a] = field[t, a]
        for q in range(nq):
            images[q] = gained[q] * inverse

        @pl.when(t == 0)
        def _():
            left_copy.wait()

        def two_terms(values):
            high = values.astype(BF16).astype(F32)
            return jnp.concatenate([high, values - high], axis=0).astype(BF16)

        arrived(field_in.at[t, c, pl.ds(0, na - 1)], field_recv.at[t, c])
        mine = two_terms(jnp.sum(field_in[t, c].astype(F32), axis=0))
        arrived(field_in.at[t, other], field_recv.at[t, other])
        theirs = two_terms(jnp.sum(field_in[t, other].astype(F32), axis=0))
        partial = jnp.zeros((8, half), F32)
        bands_at = pl.ds(pl.multiple_of(c * half, half), half)
        for k in range(4):
            out = lax.dot_general(mine, left_v[k, bands_at, :], NT, preferred_element_type=F32)
            out += lax.dot_general(theirs, left_o[k], NT, preferred_element_type=F32)
            partial = partial + jnp.where(own_k(half, k), out[0:8] + out[8:16], 0.0)
        direct[t, c, z] = partial.astype(BF16)

        @pl.loop(1, nz)
        def _(i):
            tz = z_near(nz - i)
            for n, core in enumerate((c, other)):
                pltpu.make_async_remote_copy(
                    direct.at[t, c, z], direct.at[t, c, z], direct_send.at[t, n],
                    direct_recv.at[t, c], (y, x, tz, core), device_id_type=MESH,
                ).start()

        pltpu.make_async_remote_copy(
            direct.at[t, c, z], direct.at[t, c, z], direct_send.at[t, 1],
            direct_recv.at[t, c], partner, device_id_type=MESH,
        ).start()
        arrived(direct.at[t, c, pl.ds(0, nz - 1)], direct_recv.at[t, c])
        arrived(direct.at[t, other], direct_recv.at[t, other])
        whole = jnp.concatenate(
            [jnp.sum(direct[t, h].astype(F32), axis=0) for h in range(2)], axis=1
        )

        vector = vec[...]
        applied = levels[...] * vector - whole - beta[:, 0:1] * old[...]
        cross = jnp.sum(vector * applied, axis=1, keepdims=True)
        square = jnp.sum(applied * applied, axis=1, keepdims=True)
        norm = jnp.sum(vector * vector, axis=1, keepdims=True)
        cross, square, norm = row_total(cross), row_total(square), row_total(norm)
        line = jnp.zeros((1, 128), F32)
        for n, value in enumerate((cross, square, norm)):
            line = jnp.where(lane[0:1] == n, value[0:1], line)
            line = jnp.where(lane[0:1] == n + 3, value[4:5], line)
        sums[t, a] = line
        applied_v[...] = applied

        @pl.when(t < STEPS - 1)
        def _():
            send_density(t + 1, applied - share(cross, norm) * vector)

        def send_sums(ta, ty, tx):
            pltpu.make_async_remote_copy(
                sums.at[t, a], sums.at[t, a], sums_send.at[t], sums_recv.at[t],
                (ty, tx, z, c), device_id_type=MESH,
            ).start()

        plane_sends(send_sums)

    finish(STEPS - 1)
    group = pl.ds(pl.multiple_of((b // 4) * 128, 128), 128)
    for n, source in enumerate((vec, old)):
        packed[n] = pltpu.roll(source[:, group], lax.rem(128 - lax.rem(b, 4) * 32, 128), 1)

    def sent(ref, sem):
        pltpu.make_async_copy(ref, ref, sem).wait()

    sent(pk.at[pl.ds(0, nz * 2 - 1)], pk_send.at[0])

    @pl.loop(0, STEPS)
    def _(t):
        sent(field.at[t, pl.ds(0, na - 1)], field_send.at[t, 0])
        sent(field.at[t], field_send.at[t, 1])
        sent(sums.at[t, pl.ds(0, na - 1)], sums_send.at[t])
        sent(direct.at[t, c, pl.ds(0, nz - 1)], direct_send.at[t, 0])
        sent(direct.at[t, c], direct_send.at[t, 1])

        sent(gath.at[t, c, z, pl.ds(0, na - 1)], gx_send.at[t, z])

        @pl.loop(0, nz)
        def _(tz):
            sent(gath.at[t, c, tz], fwd_send.at[t, tz])

        @pl.loop(1, 1 + 2 * NEAR)
        def _(i):
            sent(gath.at[t, c, z], gz_send.at[t, z_near(i)])

        @pl.loop(1 + 2 * NEAR, nz)
        def _(i):
            tz = z_near(i)
            sent(gath.at[t, c, tz, pl.ds(0, na - 1)], gx_send.at[t, tz])
            sent(gath.at[t, c, z, a], gz_send.at[t, tz])


def unpack(packed, last, prior, alphas, betas):
    for n, ref in ((0, last), (1, prior)):
        ref[0] = packed[n, 0:4, :32]
        ref[1] = packed[n, 4:8, :32]
    for n, ref in ((2, alphas), (3, betas)):
        ref[0:1, :] = packed[n, 0:1, :STEPS]
        ref[1:2, :] = packed[n, 4:5, :STEPS]


def on_device(
    energies, current, previous, previous_beta, pair_left, pair_right, screened, momentum_index
):
    ny, nx, nz = lax.axis_size("kpt_0"), lax.axis_size("kpt_1"), lax.axis_size("pw_0")
    na = ny * nx
    nvec = current.shape[0]
    bands, width = pair_left.shape[1:]
    nq = screened.shape[0]
    dma = pltpu.SemaphoreType.DMA
    vmem = pl.BlockSpec(memory_space=pltpu.VMEM)
    hbm = pl.BlockSpec(memory_space=pl.ANY)
    packed = pl.pallas_call(
        functools.partial(kernel, (ny, nx, nz)),
        out_shape=jax.ShapeDtypeStruct((4, 8, 128), F32),
        in_specs=[hbm] * 8,
        out_specs=vmem,
        scratch_shapes=[
            pltpu.VMEM(energies.shape, F32),
            pltpu.VMEM(current.shape, F32),
            pltpu.VMEM(previous.shape, F32),
            pltpu.SMEM(previous_beta.shape, F32),
            pltpu.VMEM(momentum_index.shape, jnp.int32),
            pltpu.VMEM(pair_left.shape, BF16),
            pltpu.VMEM(pair_right.shape, BF16),
            pltpu.VMEM((2, nz, nq, width, width), BF16),
            pltpu.VMEM((na * 8, nq * na * 8), BF16),
            pltpu.VMEM((4, bands // 2, width), BF16),
            pltpu.VMEM((nz * 2, 8, 128), F32),
            pltpu.VMEM((STEPS, 2, nz, na, 8, width), BF16),
            pltpu.VMEM((nq, na * 8, width), F32),
            pltpu.VMEM((nq, na * 8, width), F32),
            pltpu.VMEM((STEPS, na, 8, width), BF16),
            pltpu.VMEM((STEPS, 2, na, 8, width), BF16),
            pltpu.VMEM((STEPS, 2, nz, 8, bands // 2), BF16),
            pltpu.VMEM((STEPS, na, 1, 128), F32),
            pltpu.VMEM((8, bands), F32),
            pltpu.VMEM((8, bands), F32),
            pltpu.VMEM((8, bands), F32),
            pltpu.VMEM((8, 128), F32),
            pltpu.VMEM((8, bands), F32),
            pltpu.VMEM((na * 8, 128), F32),
            pltpu.VMEM((na * 8, 128), F32),
            dma((5,)),
            dma((2 + 2 * nz,)),
            dma((1,)),
            dma((1,)),
            dma((STEPS, nz)),
            dma((STEPS, nz)),
            dma((STEPS, nz)),
            dma((STEPS, nz)),
            dma((STEPS, nz)),
            dma((STEPS, nz)),
            dma((STEPS, 2)),
            dma((STEPS, 2)),
            dma((STEPS, 2)),
            dma((STEPS, 2)),
            dma((STEPS,)),
            dma((STEPS,)),
            dma(()),
            dma(()),
        ],
        compiler_params=pltpu.CompilerParams(
            collective_id=0, has_side_effects=True, vmem_limit_bytes=60 * 1024 * 1024
        ),
    )(
        energies, current, previous, previous_beta, momentum_index, pair_left, pair_right, screened
    )
    return tuple(
        pl.pallas_call(
            unpack,
            out_shape=(
                jax.ShapeDtypeStruct(current.shape, F32),
                jax.ShapeDtypeStruct(current.shape, F32),
                jax.ShapeDtypeStruct((nvec, STEPS), F32),
                jax.ShapeDtypeStruct((nvec, STEPS), F32),
            ),
            in_specs=[vmem],
            out_specs=(vmem, vmem, vmem, vmem),
        )(packed)
    )


def solution(mesh):
    kpt, pw = mesh.devices.shape
    ny = 4 if kpt % 4 == 0 else kpt
    finer = Mesh(
        mesh.devices.reshape(ny, kpt // ny, pw // 2, 2), ("kpt_0", "kpt_1", "pw_0", "pw_1")
    )
    in_specs = (
        P(KPT, PW),
        P(None, KPT, PW),
        P(None, KPT, PW),
        P(),
        P(KPT, None, PW),
        P(KPT, None, PW),
        P(KPT, PW, None),
        P(),
    )
    out_specs = (P(None, KPT, PW), P(None, KPT, PW), P(), P())
    return jax.shard_map(
        on_device, mesh=finer, in_specs=in_specs, out_specs=out_specs, check_vma=False
    )
```

```python
import functools

import jax
import jax.numpy as jnp
from jax import lax
from jax.experimental import pallas as pl
from jax.experimental.pallas import tpu as pltpu
from jax.sharding import Mesh
from jax.sharding import PartitionSpec as P

STEPS = 3
NEAR = 1
KPT = ("kpt_0", "kpt_1")
PW = ("pw_0", "pw_1")
MESH = pl.DeviceIdType.MESH
F32 = jnp.float32
BF16 = jnp.bfloat16
NT = (((1,), (1,)), ((), ()))

epsilon = 1e-06


def kernel(
    sizes, energies, current, previous, first_beta, momentum_h, left, right, screened,
    packed,
    energies_v, current_v, previous_v, first_beta_s, momentum,
    left_v, right_v, screened_v, selector,
    left_o, rows, pk, gath, gained, images, field, field_in, direct, sums,
    vec, old, levels, beta, applied_v, rest_v, inverse_v,
    small_sem, load_sem, pk_send, pk_recv, gz_send, gz_recv, gx_send, gx_recv, fwd_send, fwd_recv,
    field_send, field_recv, direct_send, direct_recv, sums_send, sums_recv, left_send, left_recv,
):
    ny, nx, nz = sizes
    na = ny * nx
    nq, width = screened.shape[0], screened.shape[1]
    bands = left.shape[1]
    half = bands // 2
    entries = momentum.shape[0] * bands
    y, x = lax.axis_index("kpt_0"), lax.axis_index("kpt_1")
    z, c = lax.axis_index("pw_0"), lax.axis_index("pw_1")
    other = 1 - c
    a = y * nx + x
    b = z * 2 + c

    tys = [lax.rem(y + d, ny) for d in range(ny)]
    txs = [lax.rem(x + d, nx) for d in range(nx)]
    far_first = sorted(
        ((dy, dx) for dy in range(ny) for dx in range(nx) if dy or dx),
        key=lambda d: -min(d[0], ny - d[0]) - min(d[1], nx - d[1]),
    )

    def plane_sends(send):
        for dy, dx in far_first:
            send(tys[dy] * nx + txs[dx], tys[dy], txs[dx])

    def plane_source(i):
        ty = lax.rem(y + ny - i // nx, ny)
        tx = lax.rem(x + nx - lax.rem(i, nx), nx)
        return ty * nx + tx

    def z_near(i):
        far, odd = (i + 1) // 2, lax.rem(i, 2)
        return lax.rem(z + odd * far + (1 - odd) * (nz - far), nz)

    def z_fixed(i):
        far = (i + 1) // 2
        return lax.rem(z + (far if i % 2 else nz - far), nz)

    partner = (y, x, z, other)

    small = [
        pltpu.make_async_copy(source, target, small_sem.at[n])
        for n, (source, target) in enumerate(
            (
                (current, current_v),
                (previous, previous_v),
                (energies, energies_v),
                (first_beta, first_beta_s),
                (momentum_h, momentum),
            )
        )
    ]
    loads = [
        pltpu.make_async_copy(right, right_v, load_sem.at[0]),
        pltpu.make_async_copy(left, left_v, load_sem.at[1]),
    ]
    for h in range(2):
        for t in range(nz):
            at = (t * 2 + h) * width
            loads.append(
                pltpu.make_async_copy(
                    screened.at[:, :, pl.ds(at, width)],
                    screened_v.at[h, t],
                    load_sem.at[2 + h * nz + t],
                )
            )
    for copy in small + loads:
        copy.start()

    barrier = pltpu.get_barrier_semaphore()

    def greet(device):
        pl.semaphore_signal(barrier, inc=1, device_id=device, device_id_type=MESH)

    @pl.loop(1, nz)
    def _(i):
        tz = z_near(nz - i)
        greet((y, x, tz, c))
        greet((y, x, tz, other))

    def greet_both(ta, ty, tx):
        greet((ty, tx, z, c))
        greet((ty, tx, z, other))

    plane_sends(greet_both)
    greet(partner)

    for copy in small:
        copy.wait()
    blank = jnp.zeros((4, 32), F32)
    for n in range(2):
        pk[b, n * 4 : n * 4 + 4, :] = jnp.concatenate(
            [current_v[n], previous_v[n], energies_v[...], blank], axis=1
        )

    nr = na * 8
    nk = momentum.shape[0]
    row = lax.broadcasted_iota(jnp.int32, (nr, nk), 0)
    col = lax.broadcasted_iota(jnp.int32, (nr, nk), 1)
    spread = ((row // 8) * 4 + row % 4 == col).astype(F32).astype(BF16)
    index = momentum[...].astype(F32).astype(BF16)
    by_row = jnp.dot(spread, index, preferred_element_type=F32).astype(BF16)
    by_both = lax.dot_general(by_row, spread, NT, preferred_element_type=F32).astype(jnp.int32)
    r1 = lax.broadcasted_iota(jnp.int32, (nr, nr), 0)
    r2 = lax.broadcasted_iota(jnp.int32, (nr, nr), 1)
    same = (r1 // 4) % 2 == (r2 // 4) % 2
    for q in range(nq):
        hit = jnp.logical_and(by_both == a * nq + q, same)
        selector[:, q * nr : (q + 1) * nr] = jnp.where(hit, 1.0, 0.0).astype(BF16)

    pl.semaphore_wait(barrier, 2 * (na - 1) + nz * 2 - 1)

    left_copy = pltpu.make_async_remote_copy(
        left_v.at[:, pl.ds(pl.multiple_of(other * half, half), half), :], left_o,
        left_send, left_recv, partner, device_id_type=MESH,
    )

    def arrived(ref, sem):
        pltpu.make_async_copy(ref, ref, sem).wait()

    def send_pk(n, device):
        pltpu.make_async_remote_copy(
            pk.at[b], pk.at[b], pk_send.at[n], pk_recv.at[0], device, device_id_type=MESH
        ).start()

    @pl.loop(1, nz)
    def _(i):
        tz = z_near(nz - i)
        send_pk(0, (y, x, tz, c))
        send_pk(0, (y, x, tz, other))

    send_pk(0, partner)
    arrived(pk.at[pl.ds(0, nz * 2 - 1)], pk_recv.at[0])

    lane = lax.broadcasted_iota(jnp.int32, (8, 128), 1)
    for j in range(bands // 128):
        for field_at, ref in ((0, vec), (1, old), (2, levels)):
            total = jnp.zeros((8, 128), F32)
            for m in range(4):
                turned = pk[4 * j + m]
                shift = (32 * (m - field_at)) % 128
                if shift:
                    turned = pltpu.roll(turned, shift, 1)
                total = total + jnp.where(lane // 32 == m, turned, 0.0)
            ref[:, j * 128 : (j + 1) * 128] = total
    upper = lax.broadcasted_iota(jnp.int32, (8, 128), 0) < 4
    beta[...] = jnp.where(upper, first_beta_s[0], first_beta_s[1])

    def own_k(n, k):
        return lax.broadcasted_iota(jnp.int32, (8, n), 0) % 4 == k

    def row_total(column):
        first = lax.broadcasted_iota(jnp.int32, (8, 1), 0) < 4
        top = jnp.sum(jnp.where(first, column, 0.0), axis=0, keepdims=True)
        low = jnp.sum(jnp.where(first, 0.0, column), axis=0, keepdims=True)
        return jnp.where(first, top, low)

    def share(cross, norm):
        some = norm > 1e-30
        return jnp.where(some, cross / jnp.where(some, norm, 1.0), 0.0)

    def to_plane(t, tz):
        def send(ta, ty, tx):
            pltpu.make_async_remote_copy(
                gath.at[t, c, tz, a], gath.at[t, c, tz, a], gx_send.at[t, tz], gx_recv.at[t, tz],
                (ty, tx, z, c), device_id_type=MESH,
            ).start()

        plane_sends(send)

    def send_density(t, values):
        high = values.astype(BF16).astype(F32)
        both = jnp.concatenate([high, values - high], axis=0).astype(BF16)
        total = jnp.zeros((8, width), F32)
        for k in range(4):
            out = jnp.dot(both, right_v[k], preferred_element_type=F32)
            total = total + jnp.where(own_k(width, k), out[0:8] + out[8:16], 0.0)
        gath[t, c, z, a] = total.astype(BF16)

        @pl.loop(1, nz - 2 * NEAR)
        def _(i):
            tz = z_near(nz - i)
            pltpu.make_async_remote_copy(
                gath.at[t, c, z, a], gath.at[t, c, z, a], gz_send.at[t, tz], gz_recv.at[t, z],
                (y, x, tz, c), device_id_type=MESH,
            ).start()

        to_plane(t, z)

    def gain(t, blocks, first=False):
        for n, (h, tz) in enumerate(blocks):
            rows[n] = gath[t, h, tz].astype(F32).reshape(nr, width).astype(BF16)
        for q in range(nq):
            total = None if first else gained[q]
            for n, (h, tz) in enumerate(blocks):
                out = lax.dot_general(
                    rows[n], screened_v[h, tz, q], NT, preferred_element_type=F32
                )
                total = out if total is None else total + out
            gained[q] = total

    def finish(t):
        arrived(sums.at[t, pl.ds(0, na - 1)], sums_recv.at[t])
        def by_row(lines, at):
            first = lax.broadcasted_iota(jnp.int32, (*lines.shape[:-2], 8, 1), lines.ndim - 2) < 4
            return jnp.where(first, lines[..., at : at + 1], lines[..., at + 3 : at + 4])

        total = jnp.sum(sums[t], axis=0)
        cross_mean = by_row(total, 0) / entries
        square_mean = by_row(total, 1) / entries
        norm_mean = by_row(total, 2) / entries
        alpha = cross_mean
        mean_square = square_mean - 2.0 * alpha * cross_mean + alpha * alpha * norm_mean
        scale = jnp.sqrt(jnp.maximum(mean_square, 0.0) + epsilon)
        vector = vec[...]
        old[...] = vector
        vec[...] = (applied_v[...] - alpha * vector) / scale
        beta[...] = jnp.broadcast_to(scale, (8, 128))
        packed[2] = jnp.where(lane == t, alpha, packed[2])
        packed[3] = jnp.where(lane == t, scale, packed[3])
        every = sums[t]
        shares = share(by_row(every, 0), by_row(every, 2))
        rest_v[...] = jnp.broadcast_to(alpha[None] - shares, (na, 8, 128)).reshape(nr, 128)
        inverse_v[...] = jnp.broadcast_to((1.0 / scale)[None], (na, 8, 128)).reshape(nr, 128)

    packed[2] = jnp.zeros((8, 128), F32)
    packed[3] = jnp.zeros((8, 128), F32)
    rest_v[...] = jnp.zeros_like(rest_v)
    inverse_v[...] = jnp.ones_like(inverse_v)
    loads[0].wait()
    send_density(0, vec[...])
    loads[1].wait()
    left_copy.start()

    @pl.loop(0, STEPS)
    def _(t):
        @pl.loop(1 + 2 * NEAR, nz)
        def _(i):
            tz = z_near(i)
            arrived(gath.at[t, c, tz, a], gz_recv.at[t, tz])
            to_plane(t, tz)

        @pl.when(t == 0)
        def _():
            for copy in loads[2:]:
                copy.wait()

        def forward(tz):
            pltpu.make_async_remote_copy(
                gath.at[t, c, tz], gath.at[t, c, tz], fwd_send.at[t, tz], fwd_recv.at[t, tz],
                partner, device_id_type=MESH,
            ).start()

        arrived(gath.at[t, c, z, pl.ds(0, na - 1)], gx_recv.at[t, z])

        @pl.loop(1, 1 + 2 * NEAR)
        def _(i):
            tz = z_near(i)
            pltpu.make_async_remote_copy(
                gath.at[t, c, z], gath.at[t, c, z], gz_send.at[t, tz], gz_recv.at[t, z],
                (y, x, tz, c), device_id_type=MESH,
            ).start()

        forward(z)
        gain(t, [(c, z)], first=True)
        batches = [
            [z_fixed(i) for i in range(1, min(5, nz))],
            [z_fixed(i) for i in range(5, nz)],
        ]
        arrived(gath.at[t, other, z], fwd_recv.at[t, z])
        gain(t, [(other, z)])

        @pl.when(t > 0)
        def _():
            finish(t - 1)
            for q in range(nq):
                gained[q] = gained[q] - rest_v[:, 0:1] * images[q]

        at = 1
        for batch in batches:
            for tz in batch:
                if at <= 2 * NEAR:
                    arrived(gath.at[t, c, tz], gz_recv.at[t, tz])
                else:
                    arrived(gath.at[t, c, tz, pl.ds(0, na - 1)], gx_recv.at[t, tz])
                forward(tz)
                at += 1
            if batch:
                gain(t, [(c, tz) for tz in batch])
        for batch in batches:
            for tz in batch:
                arrived(gath.at[t, other, tz], fwd_recv.at[t, tz])
            if batch:
                gain(t, [(other, tz) for tz in batch])

        values = gained[...].reshape(nq * nr, width)
        high = values.astype(BF16)
        low = (values - high.astype(F32)).astype(BF16)
        chosen = jnp.dot(selector[...], high, preferred_element_type=F32)
        chosen = chosen + jnp.dot(selector[...], low, preferred_element_type=F32)
        inverse = inverse_v[:, 0:1]
        field[t] = (chosen * inverse).reshape(na, 8, width).astype(BF16)

        def send_field(ta, ty, tx):
            for n, core in enumerate((c, other)):
                pltpu.make_async_remote_copy(
                    field.at[t, ta], field_in.at[t, c, a], field_send.at[t, n],
                    field_recv.at[t, c], (ty, tx, z, core), device_id_type=MESH,
                ).start()

        plane_sends(send_field)
        pltpu.make_async_remote_copy(
            field.at[t, a], field_in.at[t, c, a], field_send.at[t, 1],
            field_recv.at[t, c], partner, device_id_type=MESH,
        ).start()
        field_in[t, c, a] = field[t, a]
        for q in range(nq):
            images[q] = gained[q] * inverse

        @pl.when(t == 0)
        def _():
            left_copy.wait()

        def two_terms(values):
            high = values.astype(BF16).astype(F32)
            return jnp.concatenate([high, values - high], axis=0).astype(BF16)

        arrived(field_in.at[t, c, pl.ds(0, na - 1)], field_recv.at[t, c])
        mine = two_terms(jnp.sum(field_in[t, c].astype(F32), axis=0))
        arrived(field_in.at[t, other], field_recv.at[t, other])
        theirs = two_terms(jnp.sum(field_in[t, other].astype(F32), axis=0))
        partial = jnp.zeros((8, half), F32)
        bands_at = pl.ds(pl.multiple_of(c * half, half), half)
        for k in range(4):
            out = lax.dot_general(mine, left_v[k, bands_at, :], NT, preferred_element_type=F32)
            out += lax.dot_general(theirs, left_o[k], NT, preferred_element_type=F32)
            partial = partial + jnp.where(own_k(half, k), out[0:8] + out[8:16], 0.0)
        direct[t, c, z] = partial.astype(BF16)

        @pl.loop(1, nz)
        def _(i):
            tz = z_near(nz - i)
            for n, core in enumerate((c, other)):
                pltpu.make_async_remote_copy(
                    direct.at[t, c, z], direct.at[t, c, z], direct_send.at[t, n],
                    direct_recv.at[t, c], (y, x, tz, core), device_id_type=MESH,
                ).start()

        pltpu.make_async_remote_copy(
            direct.at[t, c, z], direct.at[t, c, z], direct_send.at[t, 1],
            direct_recv.at[t, c], partner, device_id_type=MESH,
        ).start()
        arrived(direct.at[t, c, pl.ds(0, nz - 1)], direct_recv.at[t, c])
        arrived(direct.at[t, other], direct_recv.at[t, other])
        whole = jnp.concatenate(
            [jnp.sum(direct[t, h].astype(F32), axis=0) for h in range(2)], axis=1
        )

        vector = vec[...]
        applied = levels[...] * vector - whole - beta[:, 0:1] * old[...]
        cross = jnp.sum(vector * applied, axis=1, keepdims=True)
        square = jnp.sum(applied * applied, axis=1, keepdims=True)
        norm = jnp.sum(vector * vector, axis=1, keepdims=True)
        cross, square, norm = row_total(cross), row_total(square), row_total(norm)
        line = jnp.zeros((1, 128), F32)
        for n, value in enumerate((cross, square, norm)):
            line = jnp.where(lane[0:1] == n, value[0:1], line)
            line = jnp.where(lane[0:1] == n + 3, value[4:5], line)
        sums[t, a] = line
        applied_v[...] = applied

        @pl.when(t < STEPS - 1)
        def _():
            send_density(t + 1, applied - share(cross, norm) * vector)

        def send_sums(ta, ty, tx):
            pltpu.make_async_remote_copy(
                sums.at[t, a], sums.at[t, a], sums_send.at[t], sums_recv.at[t],
                (ty, tx, z, c), device_id_type=MESH,
            ).start()

        plane_sends(send_sums)

    finish(STEPS - 1)
    group = pl.ds(pl.multiple_of((b // 4) * 128, 128), 128)
    for n, source in enumerate((vec, old)):
        packed[n] = pltpu.roll(source[:, group], lax.rem(128 - lax.rem(b, 4) * 32, 128), 1)

    def sent(ref, sem):
        pltpu.make_async_copy(ref, ref, sem).wait()

    sent(pk.at[pl.ds(0, nz * 2 - 1)], pk_send.at[0])

    @pl.loop(0, STEPS)
    def _(t):
        sent(field.at[t, pl.ds(0, na - 1)], field_send.at[t, 0])
        sent(field.at[t], field_send.at[t, 1])
        sent(sums.at[t, pl.ds(0, na - 1)], sums_send.at[t])
        sent(direct.at[t, c, pl.ds(0, nz - 1)], direct_send.at[t, 0])
        sent(direct.at[t, c], direct_send.at[t, 1])

        sent(gath.at[t, c, z, pl.ds(0, na - 1)], gx_send.at[t, z])

        @pl.loop(0, nz)
        def _(tz):
            sent(gath.at[t, c, tz], fwd_send.at[t, tz])

        @pl.loop(1, 1 + 2 * NEAR)
        def _(i):
            sent(gath.at[t, c, z], gz_send.at[t, z_near(i)])

        @pl.loop(1 + 2 * NEAR, nz)
        def _(i):
            tz = z_near(i)
            sent(gath.at[t, c, tz, pl.ds(0, na - 1)], gx_send.at[t, tz])
            sent(gath.at[t, c, z, a], gz_send.at[t, tz])


def unpack(packed, last, prior, alphas, betas):
    for n, ref in ((0, last), (1, prior)):
        ref[0] = packed[n, 0:4, :32]
        ref[1] = packed[n, 4:8, :32]
    for n, ref in ((2, alphas), (3, betas)):
        ref[0:1, :] = packed[n, 0:1, :STEPS]
        ref[1:2, :] = packed[n, 4:5, :STEPS]


def on_device(
    energies, current, previous, previous_beta, pair_left, pair_right, screened, momentum_index
):
    ny, nx, nz = lax.axis_size("kpt_0"), lax.axis_size("kpt_1"), lax.axis_size("pw_0")
    na = ny * nx
    nvec = current.shape[0]
    bands, width = pair_left.shape[1:]
    nq = screened.shape[0]
    dma = pltpu.SemaphoreType.DMA
    vmem = pl.BlockSpec(memory_space=pltpu.VMEM)
    hbm = pl.BlockSpec(memory_space=pl.ANY)
    packed = pl.pallas_call(
        functools.partial(kernel, (ny, nx, nz)),
        out_shape=jax.ShapeDtypeStruct((4, 8, 128), F32),
        in_specs=[hbm] * 8,
        out_specs=vmem,
        scratch_shapes=[
            pltpu.VMEM(energies.shape, F32),
            pltpu.VMEM(current.shape, F32),
            pltpu.VMEM(previous.shape, F32),
            pltpu.SMEM(previous_beta.shape, F32),
            pltpu.VMEM(momentum_index.shape, jnp.int32),
            pltpu.VMEM(pair_left.shape, BF16),
            pltpu.VMEM(pair_right.shape, BF16),
            pltpu.VMEM((2, nz, nq, width, width), BF16),
            pltpu.VMEM((na * 8, nq * na * 8), BF16),
            pltpu.VMEM((4, bands // 2, width), BF16),
            pltpu.VMEM((4, na * 8, width), BF16),
            pltpu.VMEM((nz * 2, 8, 128), F32),
            pltpu.VMEM((STEPS, 2, nz, na, 8, width), BF16),
            pltpu.VMEM((nq, na * 8, width), F32),
            pltpu.VMEM((nq, na * 8, width), F32),
            pltpu.VMEM((STEPS, na, 8, width), BF16),
            pltpu.VMEM((STEPS, 2, na, 8, width), BF16),
            pltpu.VMEM((STEPS, 2, nz, 8, bands // 2), BF16),
            pltpu.VMEM((STEPS, na, 1, 128), F32),
            pltpu.VMEM((8, bands), F32),
            pltpu.VMEM((8, bands), F32),
            pltpu.VMEM((8, bands), F32),
            pltpu.VMEM((8, 128), F32),
            pltpu.VMEM((8, bands), F32),
            pltpu.VMEM((na * 8, 128), F32),
            pltpu.VMEM((na * 8, 128), F32),
            dma((5,)),
            dma((2 + 2 * nz,)),
            dma((1,)),
            dma((1,)),
            dma((STEPS, nz)),
            dma((STEPS, nz)),
            dma((STEPS, nz)),
            dma((STEPS, nz)),
            dma((STEPS, nz)),
            dma((STEPS, nz)),
            dma((STEPS, 2)),
            dma((STEPS, 2)),
            dma((STEPS, 2)),
            dma((STEPS, 2)),
            dma((STEPS,)),
            dma((STEPS,)),
            dma(()),
            dma(()),
        ],
        compiler_params=pltpu.CompilerParams(
            collective_id=0, has_side_effects=True, vmem_limit_bytes=60 * 1024 * 1024
        ),
    )(
        energies, current, previous, previous_beta, momentum_index, pair_left, pair_right, screened
    )
    return tuple(
        pl.pallas_call(
            unpack,
            out_shape=(
                jax.ShapeDtypeStruct(current.shape, F32),
                jax.ShapeDtypeStruct(current.shape, F32),
                jax.ShapeDtypeStruct((nvec, STEPS), F32),
                jax.ShapeDtypeStruct((nvec, STEPS), F32),
            ),
            in_specs=[vmem],
            out_specs=(vmem, vmem, vmem, vmem),
        )(packed)
    )


def solution(mesh):
    kpt, pw = mesh.devices.shape
    ny = 4 if kpt % 4 == 0 else kpt
    finer = Mesh(
        mesh.devices.reshape(ny, kpt // ny, pw // 2, 2), ("kpt_0", "kpt_1", "pw_0", "pw_1")
    )
    in_specs = (
        P(KPT, PW),
        P(None, KPT, PW),
        P(None, KPT, PW),
        P(),
        P(KPT, None, PW),
        P(KPT, None, PW),
        P(KPT, PW, None),
        P(),
    )
    out_specs = (P(None, KPT, PW), P(None, KPT, PW), P(), P())
    return jax.shard_map(
        on_device, mesh=finer, in_specs=in_specs, out_specs=out_specs, check_vma=False
    )
```

```python
import functools

import jax
import jax.numpy as jnp
from jax import lax
from jax.experimental import pallas as pl
from jax.experimental.pallas import tpu as pltpu
from jax.sharding import Mesh
from jax.sharding import PartitionSpec as P

STEPS = 3
NEAR = 1
KPT = ("kpt_0", "kpt_1")
PW = ("pw_0", "pw_1")
MESH = pl.DeviceIdType.MESH
F32 = jnp.float32
BF16 = jnp.bfloat16
NT = (((1,), (1,)), ((), ()))

epsilon = 1e-06


def kernel(
    sizes, energies, current, previous, first_beta, momentum_h, left, right, screened,
    packed,
    energies_v, current_v, previous_v, first_beta_s, momentum,
    left_v, right_v, screened_v, selector,
    left_o, rows, pk, gath, gained, images, field, field_in, direct, sums,
    vec, old, levels, beta, applied_v, rest_v, inverse_v,
    small_sem, load_sem, pk_send, pk_recv, gz_send, gz_recv, gx_send, gx_recv, fwd_send, fwd_recv,
    field_send, field_recv, direct_send, direct_recv, sums_send, sums_recv, left_send, left_recv,
):
    ny, nx, nz = sizes
    na = ny * nx
    nq, width = screened.shape[0], screened.shape[1]
    bands = left.shape[1]
    half = bands // 2
    entries = momentum.shape[0] * bands
    y, x = lax.axis_index("kpt_0"), lax.axis_index("kpt_1")
    z, c = lax.axis_index("pw_0"), lax.axis_index("pw_1")
    other = 1 - c
    a = y * nx + x
    b = z * 2 + c

    tys = [lax.rem(y + d, ny) for d in range(ny)]
    txs = [lax.rem(x + d, nx) for d in range(nx)]
    far_first = sorted(
        ((dy, dx) for dy in range(ny) for dx in range(nx) if dy or dx),
        key=lambda d: -min(d[0], ny - d[0]) - min(d[1], nx - d[1]),
    )

    def plane_sends(send):
        for dy, dx in far_first:
            send(tys[dy] * nx + txs[dx], tys[dy], txs[dx])

    def plane_source(i):
        ty = lax.rem(y + ny - i // nx, ny)
        tx = lax.rem(x + nx - lax.rem(i, nx), nx)
        return ty * nx + tx

    def z_near(i):
        far, odd = (i + 1) // 2, lax.rem(i, 2)
        return lax.rem(z + odd * far + (1 - odd) * (nz - far), nz)

    def z_fixed(i):
        far = (i + 1) // 2
        return lax.rem(z + (far if i % 2 else nz - far), nz)

    partner = (y, x, z, other)

    small = [
        pltpu.make_async_copy(source, target, small_sem.at[n])
        for n, (source, target) in enumerate(
            (
                (current, current_v),
                (previous, previous_v),
                (energies, energies_v),
                (first_beta, first_beta_s),
                (momentum_h, momentum),
            )
        )
    ]
    loads = [
        pltpu.make_async_copy(right, right_v, load_sem.at[0]),
        pltpu.make_async_copy(left, left_v, load_sem.at[1]),
    ]
    for h in range(2):
        for t in range(nz):
            at = (t * 2 + h) * width
            loads.append(
                pltpu.make_async_copy(
                    screened.at[:, :, pl.ds(at, width)],
                    screened_v.at[h, t],
                    load_sem.at[2 + h * nz + t],
                )
            )
    for copy in small + loads:
        copy.start()

    barrier = pltpu.get_barrier_semaphore()

    def greet(device):
        pl.semaphore_signal(barrier, inc=1, device_id=device, device_id_type=MESH)

    @pl.loop(1, nz)
    def _(i):
        tz = z_near(nz - i)
        greet((y, x, tz, c))
        greet((y, x, tz, other))

    def greet_both(ta, ty, tx):
        greet((ty, tx, z, c))
        greet((ty, tx, z, other))

    plane_sends(greet_both)
    greet(partner)

    for copy in small:
        copy.wait()
    blank = jnp.zeros((4, 32), F32)
    for n in range(2):
        pk[b, n * 4 : n * 4 + 4, :] = jnp.concatenate(
            [current_v[n], previous_v[n], energies_v[...], blank], axis=1
        )

    nr = na * 8
    nk = momentum.shape[0]
    row = lax.broadcasted_iota(jnp.int32, (nr, nk), 0)
    col = lax.broadcasted_iota(jnp.int32, (nr, nk), 1)
    spread = ((row // 8) * 4 + row % 4 == col).astype(F32).astype(BF16)
    index = momentum[...].astype(F32).astype(BF16)
    by_row = jnp.dot(spread, index, preferred_element_type=F32).astype(BF16)
    by_both = lax.dot_general(by_row, spread, NT, preferred_element_type=F32).astype(jnp.int32)
    r1 = lax.broadcasted_iota(jnp.int32, (nr, nr), 0)
    r2 = lax.broadcasted_iota(jnp.int32, (nr, nr), 1)
    same = (r1 // 4) % 2 == (r2 // 4) % 2
    for q in range(nq):
        hit = jnp.logical_and(by_both == a * nq + q, same)
        selector[:, q * nr : (q + 1) * nr] = jnp.where(hit, 1.0, 0.0).astype(BF16)

    pl.semaphore_wait(barrier, 2 * (na - 1) + nz * 2 - 1)

    left_copy = pltpu.make_async_remote_copy(
        left_v.at[:, pl.ds(pl.multiple_of(other * half, half), half), :], left_o,
        left_send, left_recv, partner, device_id_type=MESH,
    )

    def arrived(ref, sem):
        pltpu.make_async_copy(ref, ref, sem).wait()

    def send_pk(n, device):
        pltpu.make_async_remote_copy(
            pk.at[b], pk.at[b], pk_send.at[n], pk_recv.at[0], device, device_id_type=MESH
        ).start()

    @pl.loop(1, nz)
    def _(i):
        tz = z_near(nz - i)
        send_pk(0, (y, x, tz, c))
        send_pk(0, (y, x, tz, other))

    send_pk(0, partner)
    arrived(pk.at[pl.ds(0, nz * 2 - 1)], pk_recv.at[0])

    lane = lax.broadcasted_iota(jnp.int32, (8, 128), 1)
    for j in range(bands // 128):
        for field_at, ref in ((0, vec), (1, old), (2, levels)):
            total = jnp.zeros((8, 128), F32)
            for m in range(4):
                turned = pk[4 * j + m]
                shift = (32 * (m - field_at)) % 128
                if shift:
                    turned = pltpu.roll(turned, shift, 1)
                total = total + jnp.where(lane // 32 == m, turned, 0.0)
            ref[:, j * 128 : (j + 1) * 128] = total
    upper = lax.broadcasted_iota(jnp.int32, (8, 128), 0) < 4
    beta[...] = jnp.where(upper, first_beta_s[0], first_beta_s[1])

    def own_k(n, k):
        return lax.broadcasted_iota(jnp.int32, (8, n), 0) % 4 == k

    def row_total(column):
        first = lax.broadcasted_iota(jnp.int32, (8, 1), 0) < 4
        top = jnp.sum(jnp.where(first, column, 0.0), axis=0, keepdims=True)
        low = jnp.sum(jnp.where(first, 0.0, column), axis=0, keepdims=True)
        return jnp.where(first, top, low)

    def share(cross, norm):
        some = norm > 1e-30
        return jnp.where(some, cross / jnp.where(some, norm, 1.0), 0.0)

    def to_plane(t, tz):
        def send(ta, ty, tx):
            pltpu.make_async_remote_copy(
                gath.at[t, c, tz, a], gath.at[t, c, tz, a], gx_send.at[t, tz], gx_recv.at[t, tz],
                (ty, tx, z, c), device_id_type=MESH,
            ).start()

        plane_sends(send)

    def send_density(t, values):
        high = values.astype(BF16).astype(F32)
        both = jnp.concatenate([high, values - high], axis=0).astype(BF16)
        total = jnp.zeros((8, width), F32)
        for k in range(4):
            out = jnp.dot(both, right_v[k], preferred_element_type=F32)
            total = total + jnp.where(own_k(width, k), out[0:8] + out[8:16], 0.0)
        gath[t, c, z, a] = total.astype(BF16)

        for i in range(nz - 1, 2 * NEAR, -1):
            tz = z_fixed(i)
            pltpu.make_async_remote_copy(
                gath.at[t, c, z, a], gath.at[t, c, z, a], gz_send.at[t, tz], gz_recv.at[t, z],
                (y, x, tz, c), device_id_type=MESH,
            ).start()

        to_plane(t, z)

    def gain(t, blocks, first=False):
        for n, (h, tz) in enumerate(blocks):
            rows[n] = gath[t, h, tz].astype(F32).reshape(nr, width).astype(BF16)
        for q in range(nq):
            total = None if first else gained[q]
            for n, (h, tz) in enumerate(blocks):
                out = lax.dot_general(
                    rows[n], screened_v[h, tz, q], NT, preferred_element_type=F32
                )
                total = out if total is None else total + out
            gained[q] = total

    def finish(t):
        arrived(sums.at[t, pl.ds(0, na - 1)], sums_recv.at[t])
        def by_row(lines, at):
            first = lax.broadcasted_iota(jnp.int32, (*lines.shape[:-2], 8, 1), lines.ndim - 2) < 4
            return jnp.where(first, lines[..., at : at + 1], lines[..., at + 3 : at + 4])

        total = jnp.sum(sums[t], axis=0)
        cross_mean = by_row(total, 0) / entries
        square_mean = by_row(total, 1) / entries
        norm_mean = by_row(total, 2) / entries
        alpha = cross_mean
        mean_square = square_mean - 2.0 * alpha * cross_mean + alpha * alpha * norm_mean
        scale = jnp.sqrt(jnp.maximum(mean_square, 0.0) + epsilon)
        vector = vec[...]
        old[...] = vector
        vec[...] = (applied_v[...] - alpha * vector) / scale
        beta[...] = jnp.broadcast_to(scale, (8, 128))
        packed[2] = jnp.where(lane == t, alpha, packed[2])
        packed[3] = jnp.where(lane == t, scale, packed[3])
        every = sums[t]
        shares = share(by_row(every, 0), by_row(every, 2))
        rest_v[...] = jnp.broadcast_to(alpha[None] - shares, (na, 8, 128)).reshape(nr, 128)
        inverse_v[...] = jnp.broadcast_to((1.0 / scale)[None], (na, 8, 128)).reshape(nr, 128)

    packed[2] = jnp.zeros((8, 128), F32)
    packed[3] = jnp.zeros((8, 128), F32)
    rest_v[...] = jnp.zeros_like(rest_v)
    inverse_v[...] = jnp.ones_like(inverse_v)
    loads[0].wait()
    send_density(0, vec[...])
    loads[1].wait()
    left_copy.start()

    @pl.loop(0, STEPS)
    def _(t):
        for tz in [z_fixed(i) for i in range(1 + 2 * NEAR, nz)]:
            arrived(gath.at[t, c, tz, a], gz_recv.at[t, tz])
            to_plane(t, tz)

        @pl.when(t == 0)
        def _():
            for copy in loads[2:]:
                copy.wait()

        def forward(tz):
            pltpu.make_async_remote_copy(
                gath.at[t, c, tz], gath.at[t, c, tz], fwd_send.at[t, tz], fwd_recv.at[t, tz],
                partner, device_id_type=MESH,
            ).start()

        arrived(gath.at[t, c, z, pl.ds(0, na - 1)], gx_recv.at[t, z])

        @pl.loop(1, 1 + 2 * NEAR)
        def _(i):
            tz = z_near(i)
            pltpu.make_async_remote_copy(
                gath.at[t, c, z], gath.at[t, c, z], gz_send.at[t, tz], gz_recv.at[t, z],
                (y, x, tz, c), device_id_type=MESH,
            ).start()

        forward(z)
        gain(t, [(c, z)], first=True)
        batches = [
            [z_fixed(i) for i in range(1, min(5, nz))],
            [z_fixed(i) for i in range(5, nz)],
        ]
        arrived(gath.at[t, other, z], fwd_recv.at[t, z])
        gain(t, [(other, z)])

        @pl.when(t > 0)
        def _():
            finish(t - 1)
            for q in range(nq):
                gained[q] = gained[q] - rest_v[:, 0:1] * images[q]

        at = 1
        for batch in batches:
            for tz in batch:
                if at <= 2 * NEAR:
                    arrived(gath.at[t, c, tz], gz_recv.at[t, tz])
                else:
                    arrived(gath.at[t, c, tz, pl.ds(0, na - 1)], gx_recv.at[t, tz])
                forward(tz)
                at += 1
            if batch:
                gain(t, [(c, tz) for tz in batch])
        for batch in batches:
            for tz in batch:
                arrived(gath.at[t, other, tz], fwd_recv.at[t, tz])
            if batch:
                gain(t, [(other, tz) for tz in batch])

        values = gained[...].reshape(nq * nr, width)
        high = values.astype(BF16)
        low = (values - high.astype(F32)).astype(BF16)
        chosen = jnp.dot(selector[...], high, preferred_element_type=F32)
        chosen = chosen + jnp.dot(selector[...], low, preferred_element_type=F32)
        inverse = inverse_v[:, 0:1]
        field[t] = (chosen * inverse).reshape(na, 8, width).astype(BF16)

        def send_field(ta, ty, tx):
            for n, core in enumerate((c, other)):
                pltpu.make_async_remote_copy(
                    field.at[t, ta], field_in.at[t, c, a], field_send.at[t, n],
                    field_recv.at[t, c], (ty, tx, z, core), device_id_type=MESH,
                ).start()

        plane_sends(send_field)
        pltpu.make_async_remote_copy(
            field.at[t, a], field_in.at[t, c, a], field_send.at[t, 1],
            field_recv.at[t, c], partner, device_id_type=MESH,
        ).start()
        field_in[t, c, a] = field[t, a]
        for q in range(nq):
            images[q] = gained[q] * inverse

        @pl.when(t == 0)
        def _():
            left_copy.wait()

        def two_terms(values):
            high = values.astype(BF16).astype(F32)
            return jnp.concatenate([high, values - high], axis=0).astype(BF16)

        arrived(field_in.at[t, c, pl.ds(0, na - 1)], field_recv.at[t, c])
        mine = two_terms(jnp.sum(field_in[t, c].astype(F32), axis=0))
        partial = jnp.zeros((8, half), F32)
        bands_at = pl.ds(pl.multiple_of(c * half, half), half)
        for k in range(4):
            out = lax.dot_general(mine, left_v[k, bands_at, :], NT, preferred_element_type=F32)
            partial = partial + jnp.where(own_k(half, k), out[0:8] + out[8:16], 0.0)
        arrived(field_in.at[t, other], field_recv.at[t, other])
        theirs = two_terms(jnp.sum(field_in[t, other].astype(F32), axis=0))
        for k in range(4):
            out = lax.dot_general(theirs, left_o[k], NT, preferred_element_type=F32)
            partial = partial + jnp.where(own_k(half, k), out[0:8] + out[8:16], 0.0)
        direct[t, c, z] = partial.astype(BF16)

        for tz in [z_fixed(i) for i in range(nz - 1, 0, -1)]:
            for n, core in enumerate((c, other)):
                pltpu.make_async_remote_copy(
                    direct.at[t, c, z], direct.at[t, c, z], direct_send.at[t, n],
                    direct_recv.at[t, c], (y, x, tz, core), device_id_type=MESH,
                ).start()

        pltpu.make_async_remote_copy(
            direct.at[t, c, z], direct.at[t, c, z], direct_send.at[t, 1],
            direct_recv.at[t, c], partner, device_id_type=MESH,
        ).start()
        arrived(direct.at[t, c, pl.ds(0, nz - 1)], direct_recv.at[t, c])
        arrived(direct.at[t, other], direct_recv.at[t, other])
        whole = jnp.concatenate(
            [jnp.sum(direct[t, h].astype(F32), axis=0) for h in range(2)], axis=1
        )

        vector = vec[...]
        applied = levels[...] * vector - whole - beta[:, 0:1] * old[...]
        cross = jnp.sum(vector * applied, axis=1, keepdims=True)
        norm = jnp.sum(vector * vector, axis=1, keepdims=True)
        cross, norm = row_total(cross), row_total(norm)
        applied_v[...] = applied

        @pl.when(t < STEPS - 1)
        def _():
            send_density(t + 1, applied - share(cross, norm) * vector)

        square = row_total(jnp.sum(applied * applied, axis=1, keepdims=True))
        line = jnp.zeros((1, 128), F32)
        for n, value in enumerate((cross, square, norm)):
            line = jnp.where(lane[0:1] == n, value[0:1], line)
            line = jnp.where(lane[0:1] == n + 3, value[4:5], line)
        sums[t, a] = line

        def send_sums(ta, ty, tx):
            pltpu.make_async_remote_copy(
                sums.at[t, a], sums.at[t, a], sums_send.at[t], sums_recv.at[t],
                (ty, tx, z, c), device_id_type=MESH,
            ).start()

        plane_sends(send_sums)

    finish(STEPS - 1)
    group = pl.ds(pl.multiple_of((b // 4) * 128, 128), 128)
    for n, source in enumerate((vec, old)):
        packed[n] = pltpu.roll(source[:, group], lax.rem(128 - lax.rem(b, 4) * 32, 128), 1)

    def sent(ref, sem):
        pltpu.make_async_copy(ref, ref, sem).wait()

    sent(pk.at[pl.ds(0, nz * 2 - 1)], pk_send.at[0])

    @pl.loop(0, STEPS)
    def _(t):
        sent(field.at[t, pl.ds(0, na - 1)], field_send.at[t, 0])
        sent(field.at[t], field_send.at[t, 1])
        sent(sums.at[t, pl.ds(0, na - 1)], sums_send.at[t])
        sent(direct.at[t, c, pl.ds(0, nz - 1)], direct_send.at[t, 0])
        sent(direct.at[t, c], direct_send.at[t, 1])

        sent(gath.at[t, c, z, pl.ds(0, na - 1)], gx_send.at[t, z])

        @pl.loop(0, nz)
        def _(tz):
            sent(gath.at[t, c, tz], fwd_send.at[t, tz])

        @pl.loop(1, 1 + 2 * NEAR)
        def _(i):
            sent(gath.at[t, c, z], gz_send.at[t, z_near(i)])

        @pl.loop(1 + 2 * NEAR, nz)
        def _(i):
            tz = z_near(i)
            sent(gath.at[t, c, tz, pl.ds(0, na - 1)], gx_send.at[t, tz])
            sent(gath.at[t, c, z, a], gz_send.at[t, tz])


def unpack(packed, last, prior, alphas, betas):
    for n, ref in ((0, last), (1, prior)):
        ref[0] = packed[n, 0:4, :32]
        ref[1] = packed[n, 4:8, :32]
    for n, ref in ((2, alphas), (3, betas)):
        ref[0:1, :] = packed[n, 0:1, :STEPS]
        ref[1:2, :] = packed[n, 4:5, :STEPS]


def on_device(
    energies, current, previous, previous_beta, pair_left, pair_right, screened, momentum_index
):
    ny, nx, nz = lax.axis_size("kpt_0"), lax.axis_size("kpt_1"), lax.axis_size("pw_0")
    na = ny * nx
    nvec = current.shape[0]
    bands, width = pair_left.shape[1:]
    nq = screened.shape[0]
    dma = pltpu.SemaphoreType.DMA
    vmem = pl.BlockSpec(memory_space=pltpu.VMEM)
    hbm = pl.BlockSpec(memory_space=pl.ANY)
    packed = pl.pallas_call(
        functools.partial(kernel, (ny, nx, nz)),
        out_shape=jax.ShapeDtypeStruct((4, 8, 128), F32),
        in_specs=[hbm] * 8,
        out_specs=vmem,
        scratch_shapes=[
            pltpu.VMEM(energies.shape, F32),
            pltpu.VMEM(current.shape, F32),
            pltpu.VMEM(previous.shape, F32),
            pltpu.SMEM(previous_beta.shape, F32),
            pltpu.VMEM(momentum_index.shape, jnp.int32),
            pltpu.VMEM(pair_left.shape, BF16),
            pltpu.VMEM(pair_right.shape, BF16),
            pltpu.VMEM((2, nz, nq, width, width), BF16),
            pltpu.VMEM((na * 8, nq * na * 8), BF16),
            pltpu.VMEM((4, bands // 2, width), BF16),
            pltpu.VMEM((4, na * 8, width), BF16),
            pltpu.VMEM((nz * 2, 8, 128), F32),
            pltpu.VMEM((STEPS, 2, nz, na, 8, width), BF16),
            pltpu.VMEM((nq, na * 8, width), F32),
            pltpu.VMEM((nq, na * 8, width), F32),
            pltpu.VMEM((STEPS, na, 8, width), BF16),
            pltpu.VMEM((STEPS, 2, na, 8, width), BF16),
            pltpu.VMEM((STEPS, 2, nz, 8, bands // 2), BF16),
            pltpu.VMEM((STEPS, na, 1, 128), F32),
            pltpu.VMEM((8, bands), F32),
            pltpu.VMEM((8, bands), F32),
            pltpu.VMEM((8, bands), F32),
            pltpu.VMEM((8, 128), F32),
            pltpu.VMEM((8, bands), F32),
            pltpu.VMEM((na * 8, 128), F32),
            pltpu.VMEM((na * 8, 128), F32),
            dma((5,)),
            dma((2 + 2 * nz,)),
            dma((1,)),
            dma((1,)),
            dma((STEPS, nz)),
            dma((STEPS, nz)),
            dma((STEPS, nz)),
            dma((STEPS, nz)),
            dma((STEPS, nz)),
            dma((STEPS, nz)),
            dma((STEPS, 2)),
            dma((STEPS, 2)),
            dma((STEPS, 2)),
            dma((STEPS, 2)),
            dma((STEPS,)),
            dma((STEPS,)),
            dma(()),
            dma(()),
        ],
        compiler_params=pltpu.CompilerParams(
            collective_id=0, has_side_effects=True, vmem_limit_bytes=60 * 1024 * 1024
        ),
    )(
        energies, current, previous, previous_beta, momentum_index, pair_left, pair_right, screened
    )
    return tuple(
        pl.pallas_call(
            unpack,
            out_shape=(
                jax.ShapeDtypeStruct(current.shape, F32),
                jax.ShapeDtypeStruct(current.shape, F32),
                jax.ShapeDtypeStruct((nvec, STEPS), F32),
                jax.ShapeDtypeStruct((nvec, STEPS), F32),
            ),
            in_specs=[vmem],
            out_specs=(vmem, vmem, vmem, vmem),
        )(packed)
    )


def solution(mesh):
    kpt, pw = mesh.devices.shape
    ny = 4 if kpt % 4 == 0 else kpt
    finer = Mesh(
        mesh.devices.reshape(ny, kpt // ny, pw // 2, 2), ("kpt_0", "kpt_1", "pw_0", "pw_1")
    )
    in_specs = (
        P(KPT, PW),
        P(None, KPT, PW),
        P(None, KPT, PW),
        P(),
        P(KPT, None, PW),
        P(KPT, None, PW),
        P(KPT, PW, None),
        P(),
    )
    out_specs = (P(None, KPT, PW), P(None, KPT, PW), P(), P())
    return jax.shard_map(
        on_device, mesh=finer, in_specs=in_specs, out_specs=out_specs, check_vma=False
    )
```
